256 devices in a mesh: rows: 128 (over z, x, y), tgt: 2 (over core).
Axes of the slice: x: 4, y: 4, z: 8, core: 2. Of those that a mesh axis runs over, the one named last changes fastest.
Arguments:
- counts: int32 [128], P('rows'), may hold values from 512 to 2048, as said below
- samples: float32 [262144, 256], P('rows'), may hold values from -6 to 6
- targets: float32 [262144, 256], P('rows', 'tgt'), may hold values from -6 to 6
- point_ids: int32 [2, 512], replicated, may hold values from 0 to 262143, as said below
- block_inverse: float32 [2, 512, 512], replicated, may hold values from -4.7683716e-07 to 5.8716338e-06
Outputs:
- residual: float32 [262144, 256], P('rows', 'tgt')
The draws below stay inside these ranges and needn't reach their ends.
Inputs may be any that keep to these rules, and one draw needn't show every extreme that they name: `counts`: some device has exactly 2048 live rows. `point_ids`: every id is d * 2048 + s with s < counts[d].
All inputs are finite; a program needn't handle non-finite values.
Results may differ from the reference program's by a relative error of at most 0.0003.
Values sent between devices are 32-bit elements; how exact they have to be, the bound alone decides.
A program may use at most 64 MiB of HBM per device.

```python
import jax
import jax.numpy as jnp
from jax import lax

FEAT = 256
TARGETS = 256
BLOCK = 512
NBLK = 2
ROW_DEV = 2048
TOTAL = 262144


def shared_counts(key):
    groups = TOTAL // ROW_DEV
    drawn = jax.random.randint(jax.random.fold_in(key, 11), (groups,), ROW_DEV // 4, ROW_DEV + 1)
    fullest = jax.random.randint(jax.random.fold_in(key, 12), (), 0, groups)
    return drawn.at[fullest].set(ROW_DEV).astype(jnp.int32)


def draw_counts(key, part):
    return shared_counts(key)


def draw_point_ids(key, part):
    groups = TOTAL // ROW_DEV
    live = shared_counts(key)
    owner = jax.random.randint(jax.random.fold_in(key, 21), (NBLK, BLOCK), 0, groups)
    raw_slot = jax.random.randint(jax.random.fold_in(key, 22), (NBLK, BLOCK), 0, 1 << 20)
    slot = raw_slot % live[owner]
    return (owner * ROW_DEV + slot).astype(jnp.int32)


def draw_block_inverse(key, part):
    noise = jax.random.truncated_normal(key, -4.0, 4.0, (NBLK, BLOCK, BLOCK), jnp.float32)
    noise = noise * (1.0 / BLOCK ** 0.5)
    eye = jnp.eye(BLOCK, dtype=jnp.float32)[None]
    return ((2.0 * eye + noise) / (32.0 * (TOTAL * BLOCK) ** 0.5)).astype(jnp.float32)


def block_scale(stream_key, dims, split, least, top_value):
    loudness, own = 1.0, jax.random.fold_in(stream_key, 6)
    for dim, shards_of in split:
        steps = jnp.exp(jax.random.uniform(jax.random.fold_in(own, dim), (shards_of,), jnp.float32, least / len(split), top_value / len(split)))
        loudness = loudness * jnp.repeat(steps, dims[dim] // shards_of).reshape([-1 if axis == dim else 1 for axis in range(len(dims))])
    return loudness


def gaussian(rng, dims, width, limit, pieces=(), kind=jnp.bfloat16):
    array = jax.random.normal(rng, dims, jnp.float32) * width
    if len(pieces) > 0:
        array = block_scale(rng, dims, pieces, -0.22, 0.18) * array
    return jnp.clip(array, min=-limit, max=limit).astype(kind)


def setup_inputs(seed: int = 0) -> dict:
    keys = jax.random.split(jax.random.key(seed), 6)
    counts = draw_counts(jax.random.fold_in(keys[5], 71), 0)
    samples = gaussian(keys[1], (TOTAL, FEAT), 1.0, 6.0, ((0, 128),), jnp.float32)
    targets = gaussian(keys[2], (TOTAL, TARGETS), 1.0, 6.0, ((0, 128), (1, 2)), jnp.float32)
    point_ids = draw_point_ids(jax.random.fold_in(keys[5], 71), 0)
    block_inverse = draw_block_inverse(jax.random.fold_in(keys[5], 71), 0)
    return {"counts": counts, "samples": samples, "targets": targets, "point_ids": point_ids, "block_inverse": block_inverse}


def kernel_columns(rows_in, points):
    scaled = lax.dot_general(rows_in, points, (((1,), (1,)), ((), ())), precision=lax.Precision.HIGHEST, preferred_element_type=jnp.float32)
    scaled = scaled * (1.0 / FEAT ** 0.5)
    return (0.5 * scaled + 1.0) ** 3


def reference(counts, samples, targets, point_ids, block_inverse):
    groups = samples.shape[0] // ROW_DEV
    stacked = samples.reshape(groups, ROW_DEV, FEAT)
    alive = jnp.arange(ROW_DEV, dtype=jnp.int32)[None, :] < counts[:, None]
    residual = targets.reshape(groups, ROW_DEV, TARGETS)
    for block_index in range(NBLK):
        points = jnp.take(samples, point_ids[block_index].astype(jnp.int32), axis=0)

        def masked(rows_in, marks):
            return jnp.where(marks[:, None], kernel_columns(rows_in, points), 0.0)

        def add_sum(total, item):
            rows_in, marks, current = item
            columns = masked(rows_in, marks)
            return total + lax.dot_general(columns, current, (((0,), (0,)), ((), ())), precision=lax.Precision.HIGHEST, preferred_element_type=jnp.float32), None

        sums, unused = lax.scan(add_sum, jnp.zeros((BLOCK, TARGETS), jnp.float32), (stacked, alive, residual))
        coefs = jnp.dot(block_inverse[block_index], sums, precision=lax.Precision.HIGHEST, preferred_element_type=jnp.float32)

        def update(item):
            rows_in, marks, current = item
            return current - jnp.dot(masked(rows_in, marks), coefs, precision=lax.Precision.HIGHEST, preferred_element_type=jnp.float32)

        residual = lax.map(update, (stacked, alive, residual))
    return residual.reshape(groups * ROW_DEV, TARGETS)
```

```python
import functools

import jax
import jax.numpy as jnp
from jax import lax
from jax.experimental import pallas as pl
from jax.experimental.pallas import tpu as pltpu
from jax.sharding import Mesh
from jax.sharding import PartitionSpec as P

ROWS = ("rows_0", "rows_1", "rows_2")
MESH = pl.DeviceIdType.MESH
NZ, NX, NY = 8, 4, 4
PLANE = NX * NY
TILE = 256
NT = (((1,), (1,)), ((), ()))
NN = (((1,), (0,)), ((), ()))


def ring_hops(step, size):
    return min(step, size - step)


PLANE_STEPS = sorted(
    [(kx, ky) for kx in range(NX) for ky in range(NY) if (kx, ky) != (0, 0)],
    key=lambda k: -(ring_hops(k[0], NX) + ring_hops(k[1], NY)),
)
LINE_STEPS = sorted(range(1, NZ), key=lambda k: -ring_hops(k, NZ))


def halves(value):
    high = value.astype(jnp.bfloat16)
    low = (value - high.astype(jnp.float32)).astype(jnp.bfloat16)
    return high, low


def dot(left, right, dims):
    return lax.dot_general(left, right, dims, preferred_element_type=jnp.float32)


def kernel(
    counts, ids, samples, targets, inverse, out,
    x_high, x_low, r_turned, residual, p_high, p_low, c_high, c_low, b_high, b_low,
    p_part, p_in, p_line, p_line_in, p_full,
    s_part, s_in, s_line, s_line_in, k_full,
    send_sems, recv_sems,
):
    z, x, y = (lax.axis_index(name) for name in ROWS)
    core = lax.axis_index("tgt")
    place = x * NY + y
    other = 1 - core
    rows = samples.shape[0]
    block = ids.shape[1]
    blocks = ids.shape[0]
    mine = block // 2
    p_piece = mine // PLANE
    s_piece = targets.shape[1] // PLANE
    wide = targets.shape[1]
    tiles = rows // TILE

    def plane_peer(step):
        px, py = lax.rem(x + step[0], NX), lax.rem(y + step[1], NY)
        return (z, px, py, core), px * NY + py

    def line_peer(step):
        return (lax.rem(z + step, NZ), x, y, core)

    partner = (z, x, y, other)

    barrier = pltpu.get_barrier_semaphore()
    for step in PLANE_STEPS:
        pl.semaphore_signal(barrier, inc=1, device_id=plane_peer(step)[0], device_id_type=MESH)
    for step in LINE_STEPS:
        pl.semaphore_signal(barrier, inc=1, device_id=line_peer(step), device_id_type=MESH)
    pl.semaphore_signal(barrier, inc=1, device_id=partner, device_id_type=MESH)

    def remote(src, dst, stage, device):
        return pltpu.make_async_remote_copy(
            src_ref=src, dst_ref=dst, send_sem=send_sems.at[stage], recv_sem=recv_sems.at[stage],
            device_id=device, device_id_type=MESH,
        )

    def arrived(stage, ref):
        pltpu.make_async_copy(ref, ref, recv_sems.at[stage]).wait()

    def sent(stage, ref):
        pltpu.make_async_copy(ref, ref, send_sems.at[stage]).wait()

    def scatter_start(part, landing, size, stage):
        for slot, step in enumerate(PLANE_STEPS):
            device, index = plane_peer(step)
            start = pl.multiple_of(index * size, size)
            remote(part.at[pl.ds(start, size)], landing.at[slot], stage, device).start()

    def scatter_finish(part, landing, size, stage, line):
        arrived(stage, landing)
        total = part[pl.ds(pl.multiple_of(place * size, size), size)]
        for slot in range(PLANE - 1):
            total = total + landing[slot]
        line[...] = total

    def line_start(line, landing, stage):
        for slot, step in enumerate(LINE_STEPS):
            remote(line, landing.at[slot], stage, line_peer(step)).start()

    def line_finish(line, landing, stage):
        arrived(stage, landing)
        total = line[...]
        for slot in range(NZ - 1):
            total = total + landing[slot]
        return total

    def gather_start(full, start, size, stage):
        piece = full.at[pl.ds(start, size)]
        for step in PLANE_STEPS:
            remote(piece, piece, stage, plane_peer(step)[0]).start()

    def points_stage(b, n):
        return 5 * b + n

    def sums_stage(b, n):
        return 5 * blocks + 3 * b + n

    def split_samples(i, carry):
        at = pl.ds(pl.multiple_of(i * TILE, TILE), TILE)
        high, low = halves(samples[at])
        x_high[at] = high
        x_low[at] = low
        return carry

    lax.fori_loop(0, tiles, split_samples, 0)

    first = ((z * NX + x) * NY + y) * rows

    def pick(b):
        wanted = ids[pl.ds(b, 1), pl.ds(pl.multiple_of(core * mine, mine), mine)] - first
        column = jnp.broadcast_to(wanted.astype(jnp.float32), (8, mine)).T[:, :1]
        slots = lax.broadcasted_iota(jnp.int32, (mine, rows), 1).astype(jnp.float32)
        chosen = jnp.where(column == slots, 1.0, 0.0).astype(jnp.bfloat16)
        p_part[b] = dot(chosen, x_high[...], NN) + dot(chosen, x_low[...], NN)

    pick(0)
    pl.semaphore_wait(barrier, PLANE + NZ - 1)
    scatter_start(p_part.at[0], p_in.at[0], p_piece, points_stage(0, 0))
    pick(1)
    scatter_start(p_part.at[1], p_in.at[1], p_piece, points_stage(1, 0))

    def turn(value, i):
        at = pl.ds(pl.multiple_of(i * TILE, TILE), TILE)
        high, low = halves(value.T)
        r_turned[pl.ds(0, wide), at] = high
        r_turned[pl.ds(wide, wide), at] = low

    def turn_targets(i, carry):
        turn(targets[pl.ds(pl.multiple_of(i * TILE, TILE), TILE)], i)
        return carry

    lax.fori_loop(0, tiles, turn_targets, 0)
    for b in range(blocks):
        b_high[b], b_low[b] = halves(inverse[b])

    for b in range(blocks):
        scatter_finish(p_part.at[b], p_in.at[b], p_piece, points_stage(b, 0), p_line.at[b])
        line_start(p_line.at[b], p_line_in.at[b], points_stage(b, 1))
    own = pl.multiple_of(core * mine, mine)
    own_piece = pl.multiple_of(core * mine + place * p_piece, p_piece)
    for b in range(blocks):
        total = line_finish(p_line.at[b], p_line_in.at[b], points_stage(b, 1))
        p_full[b, pl.ds(own_piece, p_piece)] = total
        gather_start(p_full.at[b], own_piece, p_piece, points_stage(b, 2))

    def swap_halves(b):
        arrived(points_stage(b, 2), p_in.at[b])
        half = p_full.at[b, pl.ds(own, mine)]
        remote(half, half, points_stage(b, 3), partner).start()

    def points_ready(b):
        arrived(points_stage(b, 3), p_part.at[b])
        p_high[b], p_low[b] = halves(p_full[b] * (0.5 / samples.shape[1] ** 0.5))

    live = counts[0]

    def columns_tile(b, i):
        at = pl.ds(pl.multiple_of(i * TILE, TILE), TILE)
        near = (
            dot(x_high[at], p_high[b], NT)
            + dot(x_high[at], p_low[b], NT)
            + dot(x_low[at], p_high[b], NT)
        ) + 1.0
        slots = i * TILE + lax.broadcasted_iota(jnp.int32, near.shape, 0)
        high, low = halves(jnp.where(slots < live, near * near * near, 0.0))
        c_high[b, at] = high
        c_low[b, at] = low
        return high, low

    def add_sums(b, i, high, low):
        across = pl.ds(pl.multiple_of(i * TILE, TILE), TILE)
        both = dot(r_turned[:, across], high, NN)
        s_part[b] += both[:wide] + both[wide:] + dot(r_turned[pl.ds(0, wide), across], low, NN)

    def update(b, i, current):
        at = pl.ds(pl.multiple_of(i * TILE, TILE), TILE)
        coefs = k_full[b]
        c_h, c_l = halves(coefs)
        both = dot(c_high[b, at], jnp.concatenate([c_h, c_l], axis=0), NT)
        return current - (both[:, :wide] + both[:, wide:] + dot(c_low[b, at], c_h, NT))

    def sums_exchange(b):
        scatter_finish(s_part.at[b], s_in.at[b], s_piece, sums_stage(b, 0), s_line.at[b])
        line_start(s_line.at[b], s_line_in.at[b], sums_stage(b, 1))
        sums = line_finish(s_line.at[b], s_line_in.at[b], sums_stage(b, 1))
        high, low = halves(sums)
        at = pl.multiple_of(place * s_piece, s_piece)
        k_full[b, pl.ds(at, s_piece)] = (
            dot(high, b_high[b], NT) + dot(high, b_low[b], NT) + dot(low, b_high[b], NT)
        )
        gather_start(k_full.at[b], at, s_piece, sums_stage(b, 2))
        arrived(sums_stage(b, 2), s_in.at[b])

    swap_halves(0)
    points_ready(0)
    s_part[...] = jnp.zeros_like(s_part)

    def first_block(i, carry):
        add_sums(0, i, *columns_tile(0, i))
        return carry

    lax.fori_loop(0, tiles, first_block, 0)
    scatter_start(s_part.at[0], s_in.at[0], s_piece, sums_stage(0, 0))
    swap_halves(1)
    points_ready(1)

    def second_columns(i, carry):
        columns_tile(1, i)
        return carry

    lax.fori_loop(0, tiles, second_columns, 0)
    sums_exchange(0)

    def second_block(i, carry):
        at = pl.ds(pl.multiple_of(i * TILE, TILE), TILE)
        left = update(0, i, targets[at])
        residual[at] = left
        turn(left, i)
        add_sums(1, i, c_high[1, at], c_low[1, at])
        return carry

    lax.fori_loop(0, tiles, second_block, 0)
    scatter_start(s_part.at[1], s_in.at[1], s_piece, sums_stage(1, 0))
    sums_exchange(1)

    def last(i, carry):
        at = pl.ds(pl.multiple_of(i * TILE, TILE), TILE)
        out[at] = update(1, i, residual[at])
        return carry

    lax.fori_loop(0, tiles, last, 0)

    for b in range(blocks):
        sent(points_stage(b, 0), p_in.at[b])
        sent(points_stage(b, 1), p_line_in.at[b])
        sent(points_stage(b, 2), p_in.at[b])
        sent(points_stage(b, 3), p_part.at[b])
        sent(sums_stage(b, 0), s_in.at[b])
        sent(sums_stage(b, 1), s_line_in.at[b])
        sent(sums_stage(b, 2), s_in.at[b])


def on_device(counts, samples, targets, point_ids, block_inverse):
    rows, feat = samples.shape
    blocks, block = point_ids.shape
    wide = targets.shape[1]
    mine = block // 2
    p_piece, s_piece = mine // PLANE, wide // PLANE
    f32, bf16 = jnp.float32, jnp.bfloat16
    vmem = pl.BlockSpec(memory_space=pltpu.VMEM)
    return pl.pallas_call(
        kernel,
        out_shape=jax.ShapeDtypeStruct(targets.shape, f32),
        in_specs=[pl.BlockSpec(memory_space=pltpu.SMEM), vmem, vmem, vmem, vmem],
        out_specs=vmem,
        scratch_shapes=[
            pltpu.VMEM((rows, feat), bf16),
            pltpu.VMEM((rows, feat), bf16),
            pltpu.VMEM((2 * wide, rows), bf16),
            pltpu.VMEM((rows, wide), f32),
            pltpu.VMEM((blocks, block, feat), bf16),
            pltpu.VMEM((blocks, block, feat), bf16),
            pltpu.VMEM((blocks, rows, block), bf16),
            pltpu.VMEM((blocks, rows, block), bf16),
            pltpu.VMEM((blocks, block, block), bf16),
            pltpu.VMEM((blocks, block, block), bf16),
            pltpu.VMEM((blocks, mine, feat), f32),
            pltpu.VMEM((blocks, PLANE - 1, p_piece, feat), f32),
            pltpu.VMEM((blocks, p_piece, feat), f32),
            pltpu.VMEM((blocks, NZ - 1, p_piece, feat), f32),
            pltpu.VMEM((blocks, block, feat), f32),
            pltpu.VMEM((blocks, wide, block), f32),
            pltpu.VMEM((blocks, PLANE - 1, s_piece, block), f32),
            pltpu.VMEM((blocks, s_piece, block), f32),
            pltpu.VMEM((blocks, NZ - 1, s_piece, block), f32),
            pltpu.VMEM((blocks, wide, block), f32),
            pltpu.SemaphoreType.DMA((8 * blocks,)),
            pltpu.SemaphoreType.DMA((8 * blocks,)),
        ],
        compiler_params=pltpu.CompilerParams(collective_id=0, has_side_effects=True),
    )(counts, point_ids, samples, targets, block_inverse)


def solution(mesh):
    finer = Mesh(
        mesh.devices.reshape(NZ, NX, NY, mesh.shape["tgt"]), ("rows_0", "rows_1", "rows_2", "tgt")
    )
    placed = (P(ROWS), P(ROWS, None), P(ROWS, "tgt"), P(), P())
    return jax.shard_map(
        on_device, mesh=finer, in_specs=placed, out_specs=P(ROWS, "tgt"), check_vma=False
    )
```

```python
import jax
import jax.numpy as jnp
from jax import lax
from jax.experimental import pallas as pl
from jax.experimental.pallas import tpu as pltpu
from jax.sharding import Mesh
from jax.sharding import PartitionSpec as P

ROWS = ("rows_0", "rows_1", "rows_2")
MESH = pl.DeviceIdType.MESH
NZ, NX, NY = 8, 4, 4
PLANE = NX * NY
TILE = 256
CHUNKS = 4
FIRST, SECOND = 2, 6
NT = (((1,), (1,)), ((), ()))
NN = (((1,), (0,)), ((), ()))
f32, bf16 = jnp.float32, jnp.bfloat16


def ring_hops(step, size):
    return min(step, size - step)


PLANE_STEPS = sorted(
    [(kx, ky) for kx in range(NX) for ky in range(NY) if (kx, ky) != (0, 0)],
    key=lambda k: -(ring_hops(k[0], NX) + ring_hops(k[1], NY)),
)
LINE_STEPS = sorted(range(1, NZ), key=lambda k: -ring_hops(k, NZ))


def halves(value):
    high = value.astype(bf16)
    low = (value - high.astype(f32)).astype(bf16)
    return high, low


def dot(left, right, dims):
    return lax.dot_general(left, right, dims, preferred_element_type=f32)


def tile_at(i):
    return pl.ds(pl.multiple_of(i * TILE, TILE), TILE)


def kernel(
    counts, ids_in, samples_in, targets_in, inverse_in, out,
    ids, samples, targets, inverse,
    x_high, x_low, r_turned, residual, p_high, p_low, c_high, c_low, b_high, b_low,
    cross, cross_high, cross_low,
    part, landing, line, line_in, full, swapped,
    in_sems, send_sems, recv_sems,
):
    z, x, y = (lax.axis_index(name) for name in ROWS)
    core = lax.axis_index("tgt")
    place = x * NY + y
    rows = samples.shape[0]
    tiles = rows // TILE
    blocks, block = ids.shape
    mine = block // 2
    unit = part.shape[1]
    piece = unit // PLANE
    wide = targets.shape[1]

    def plane_peer(step):
        px, py = lax.rem(x + step[0], NX), lax.rem(y + step[1], NY)
        return (z, px, py, core), px * NY + py

    def line_peer(step):
        return (lax.rem(z + step, NZ), x, y, core)

    partner = (z, x, y, 1 - core)

    barrier = pltpu.get_barrier_semaphore()
    for step in PLANE_STEPS:
        pl.semaphore_signal(barrier, inc=1, device_id=plane_peer(step)[0], device_id_type=MESH)
    for step in LINE_STEPS:
        pl.semaphore_signal(barrier, inc=1, device_id=line_peer(step), device_id_type=MESH)
    pl.semaphore_signal(barrier, inc=1, device_id=partner, device_id_type=MESH)

    chunk = rows // CHUNKS
    ids_copy = pltpu.make_async_copy(ids_in, ids, in_sems.at[CHUNKS])
    targets_copy = pltpu.make_async_copy(targets_in, targets, in_sems.at[CHUNKS + 1])
    inverse_copy = pltpu.make_async_copy(inverse_in, inverse, in_sems.at[CHUNKS + 2])

    def samples_copy(n):
        at = pl.ds(n * chunk, chunk)
        return pltpu.make_async_copy(samples_in.at[at], samples.at[at], in_sems.at[n])

    ids_copy.start()
    for n in range(CHUNKS):
        samples_copy(n).start()

    def remote(src, dst, stage, device):
        return pltpu.make_async_remote_copy(
            src_ref=src, dst_ref=dst, send_sem=send_sems.at[stage], recv_sem=recv_sems.at[stage],
            device_id=device, device_id_type=MESH,
        )

    def arrived(u, n, ref):
        pltpu.make_async_copy(ref, ref, recv_sems.at[4 * u + n]).wait()

    def sent(u, n, ref):
        pltpu.make_async_copy(ref, ref, send_sems.at[4 * u + n]).wait()

    own_piece = pl.ds(pl.multiple_of(place * piece, piece), piece)

    def scatter(u):
        for slot, step in enumerate(PLANE_STEPS):
            device, index = plane_peer(step)
            src = part.at[u, pl.ds(pl.multiple_of(index * piece, piece), piece)]
            remote(src, landing.at[u, slot], 4 * u, device).start()

    def to_line(u):
        arrived(u, 0, landing.at[u])
        total = part[u, own_piece]
        for slot in range(PLANE - 1):
            total = total + landing[u, slot]
        line[u] = total
        for slot, step in enumerate(LINE_STEPS):
            remote(line.at[u], line_in.at[u, slot], 4 * u + 1, line_peer(step)).start()

    def off_line(u):
        arrived(u, 1, line_in.at[u])
        total = line[u]
        for slot in range(NZ - 1):
            total = total + line_in[u, slot]
        return total

    def gather(u, value):
        full[u, own_piece] = value
        ref = full.at[u, own_piece]
        for step in PLANE_STEPS:
            remote(ref, ref, 4 * u + 2, plane_peer(step)[0]).start()

    def gathered(u):
        arrived(u, 2, landing.at[u])

    def swap(u):
        gathered(u)
        remote(full.at[u], swapped.at[u], 4 * u + 3, partner).start()

    per_chunk = tiles // CHUNKS
    for n in range(CHUNKS):
        samples_copy(n).wait()

        def split_samples(i, carry):
            at = tile_at(i)
            x_high[at], x_low[at] = halves(samples[at])
            return carry

        lax.fori_loop(n * per_chunk, (n + 1) * per_chunk, split_samples, 0)
    targets_copy.start()
    inverse_copy.start()
    ids_copy.wait()

    first = ((z * NX + x) * NY + y) * rows

    def pick(u):
        start = pl.multiple_of(core * mine + (u % 2) * unit, unit)
        wanted = ids[pl.ds(u // 2, 1), pl.ds(start, unit)] - first
        column = jnp.broadcast_to(wanted.astype(f32), (8, unit)).T[:, :1]
        slots = lax.broadcasted_iota(jnp.int32, (unit, rows), 1).astype(f32)
        chosen = jnp.where(column == slots, 1.0, 0.0).astype(bf16)
        part[u] = dot(chosen, x_high[...], NN) + dot(chosen, x_low[...], NN)

    pick(0)
    pl.semaphore_wait(barrier, PLANE + NZ - 1)
    scatter(0)
    pick(1)
    scatter(1)
    pick(2)
    pick(3)

    targets_copy.wait()

    def turn_targets(i, carry):
        at = tile_at(i)
        high, low = halves(targets[at].T)
        r_turned[pl.ds(0, wide), at] = high
        r_turned[pl.ds(wide, wide), at] = low
        return carry

    lax.fori_loop(0, tiles, turn_targets, 0)
    to_line(0)
    to_line(1)
    scatter(2)
    scatter(3)

    inverse_copy.wait()
    for b in range(blocks):
        for i in range(2):
            for j in range(2):
                from_i = pl.ds(pl.multiple_of((core + i) % 2 * mine, mine), mine)
                from_j = pl.ds(pl.multiple_of((core + j) % 2 * mine, mine), mine)
                high, low = halves(inverse[b, from_i, from_j])
                b_high[b, pl.ds(i * mine, mine), pl.ds(j * mine, mine)] = high
                b_low[b, pl.ds(i * mine, mine), pl.ds(j * mine, mine)] = low

    gather(0, off_line(0))
    gather(1, off_line(1))
    to_line(2)
    to_line(3)

    scale = 0.5 / samples.shape[1] ** 0.5

    def points_ready(b, h):
        for n in range(2):
            u = 2 * b + n
            if h == 1:
                arrived(u, 3, swapped.at[u])
            value = swapped[u] if h == 1 else full[u]
            at = pl.ds(h * mine + n * unit, unit)
            p_high[b, at], p_low[b, at] = halves(value * scale)

    live = counts[0]

    def columns_tile(b, h, i):
        at = tile_at(i)
        points = pl.ds(h * mine, mine)
        high, low = p_high[b, points], p_low[b, points]
        near = (dot(x_high[at], high, NT) + dot(x_high[at], low, NT) + dot(x_low[at], high, NT)) + 1.0
        slots = i * TILE + lax.broadcasted_iota(jnp.int32, near.shape, 0)
        cubed = jnp.where(slots < live, near * near * near, 0.0)
        high, low = halves(cubed)
        c_high[b, at, points] = high
        c_low[b, at, points] = low
        return cubed, high, low

    def add_sums(u, i, high, low):
        across = tile_at(i)
        both = dot(r_turned[:, across], high, NN)
        part[u] += both[:wide] + both[wide:] + dot(r_turned[pl.ds(0, wide), across], low, NN)

    def update(u, i, current):
        b, h = u // 2 - blocks, u % 2
        points = pl.ds(h * mine, mine)
        high, low = halves(full[u])
        both = dot(c_high[b, tile_at(i), points], jnp.concatenate([high, low], axis=0), NT)
        return current - (both[:, :wide] + both[:, wide:] + dot(c_low[b, tile_at(i), points], high, NT))

    def coefs(b):
        first_unit = 2 * (blocks + b)
        sums = jnp.concatenate([off_line(first_unit), off_line(first_unit + 1)], axis=1)
        high, low = halves(sums)
        both = jnp.concatenate([high, low], axis=0)
        for h in range(2):
            at = pl.ds(h * mine, mine)
            value = dot(both, b_high[b, at], NT)
            gather(first_unit + h, value[:piece] + value[piece:] + dot(high, b_low[b, at], NT))

    for u in range(2 * blocks, 4 * blocks):
        part[u] = jnp.zeros_like(part[u])
    cross[...] = jnp.zeros_like(cross)

    swap(0)
    swap(1)
    points_ready(0, 0)
    gather(2, off_line(2))
    gather(3, off_line(3))

    for h in range(2):
        if h == 1:
            points_ready(0, 1)

        def first_block(i, carry):
            cubed, high, low = columns_tile(0, h, i)
            add_sums(4 + h, i, high, low)
            return carry

        lax.fori_loop(0, tiles, first_block, 0)
        scatter(4 + h)

    swap(2)
    swap(3)
    points_ready(1, 0)
    to_line(4)
    points_ready(1, 1)

    def second_columns(i, carry):
        at = tile_at(i)
        for h in range(2):
            cubed, high, low = columns_tile(1, h, i)
            add_sums(6 + h, i, high, low)
            t_high, t_low = halves(cubed.T)
            cross[pl.ds(h * mine, mine)] += (
                dot(t_high, c_high[0, at], NN) + dot(t_high, c_low[0, at], NN) + dot(t_low, c_high[0, at], NN)
            )
        return carry

    lax.fori_loop(0, FIRST, second_columns, 0)
    to_line(5)
    lax.fori_loop(FIRST, SECOND, second_columns, 0)
    coefs(0)
    lax.fori_loop(SECOND, tiles, second_columns, 0)
    cross_high[...], cross_low[...] = halves(cross[...])

    gathered(4)
    gathered(5)
    high, low = halves(jnp.concatenate([full[4], full[5]], axis=1))
    both = jnp.concatenate([high, low], axis=0)
    for h in range(2):
        at = pl.ds(h * mine, mine)
        value = dot(both, cross_high[at], NT)
        part[6 + h] -= value[:wide] + value[wide:] + dot(high, cross_low[at], NT)
        scatter(6 + h)

    def first_update(i, carry):
        at = tile_at(i)
        residual[at] = update(5, i, update(4, i, targets[at]))
        return carry

    lax.fori_loop(0, tiles, first_update, 0)
    to_line(6)
    to_line(7)
    coefs(1)
    gathered(6)

    def second_update(i, carry):
        at = tile_at(i)
        residual[at] = update(6, i, residual[at])
        return carry

    lax.fori_loop(0, tiles, second_update, 0)
    gathered(7)

    def last_update(i, carry):
        at = tile_at(i)
        out[at] = update(7, i, residual[at])
        return carry

    lax.fori_loop(0, tiles, last_update, 0)

    for u in range(4 * blocks):
        sent(u, 0, landing.at[u])
        sent(u, 1, line_in.at[u])
        sent(u, 2, landing.at[u])
        if u < 2 * blocks:
            sent(u, 3, swapped.at[u])


def on_device(counts, samples, targets, point_ids, block_inverse):
    rows, feat = samples.shape
    blocks, block = point_ids.shape
    wide = targets.shape[1]
    units, unit, lanes = 4 * blocks, block // 4, block // 2
    piece = unit // PLANE
    anywhere = pl.BlockSpec(memory_space=pl.ANY)
    return pl.pallas_call(
        kernel,
        out_shape=jax.ShapeDtypeStruct(targets.shape, f32),
        in_specs=[pl.BlockSpec(memory_space=pltpu.SMEM)] + [anywhere] * 4,
        out_specs=pl.BlockSpec(memory_space=pltpu.VMEM),
        scratch_shapes=[
            pltpu.VMEM(point_ids.shape, jnp.int32),
            pltpu.VMEM((rows, feat), f32),
            pltpu.VMEM((rows, wide), f32),
            pltpu.VMEM((blocks, block, block), f32),
            pltpu.VMEM((rows, feat), bf16),
            pltpu.VMEM((rows, feat), bf16),
            pltpu.VMEM((2 * wide, rows), bf16),
            pltpu.VMEM((rows, wide), f32),
            pltpu.VMEM((blocks, block, feat), bf16),
            pltpu.VMEM((blocks, block, feat), bf16),
            pltpu.VMEM((blocks, rows, block), bf16),
            pltpu.VMEM((blocks, rows, block), bf16),
            pltpu.VMEM((blocks, block, block), bf16),
            pltpu.VMEM((blocks, block, block), bf16),
            pltpu.VMEM((block, block), f32),
            pltpu.VMEM((block, block), bf16),
            pltpu.VMEM((block, block), bf16),
            pltpu.VMEM((units, unit, lanes), f32),
            pltpu.VMEM((units, PLANE - 1, piece, lanes), f32),
            pltpu.VMEM((units, piece, lanes), f32),
            pltpu.VMEM((units, NZ - 1, piece, lanes), f32),
            pltpu.VMEM((units, unit, lanes), f32),
            pltpu.VMEM((2 * blocks, unit, lanes), f32),
            pltpu.SemaphoreType.DMA((CHUNKS + 3,)),
            pltpu.SemaphoreType.DMA((4 * units,)),
            pltpu.SemaphoreType.DMA((4 * units,)),
        ],
        compiler_params=pltpu.CompilerParams(collective_id=0, has_side_effects=True),
    )(counts, point_ids, samples, targets, block_inverse)


def solution(mesh):
    finer = Mesh(
        mesh.devices.reshape(NZ, NX, NY, mesh.shape["tgt"]), ("rows_0", "rows_1", "rows_2", "tgt")
    )
    placed = (P(ROWS), P(ROWS, None), P(ROWS, "tgt"), P(), P())
    return jax.shard_map(
        on_device, mesh=finer, in_specs=placed, out_specs=P(ROWS, "tgt"), check_vma=False
    )
```

```python
import jax
import jax.numpy as jnp
from jax import lax
from jax.experimental import pallas as pl
from jax.experimental.pallas import tpu as pltpu
from jax.sharding import Mesh
from jax.sharding import PartitionSpec as P

ROWS = ("rows_0", "rows_1", "rows_2")
MESH = pl.DeviceIdType.MESH
NZ, NX, NY = 8, 4, 4
PLANE = NX * NY
TILE = 256
CHUNKS = 4
NT = (((1,), (1,)), ((), ()))
NN = (((1,), (0,)), ((), ()))
f32, bf16 = jnp.float32, jnp.bfloat16


def ring_hops(step, size):
    return min(step, size - step)


PLANE_STEPS = sorted(
    [(kx, ky) for kx in range(NX) for ky in range(NY) if (kx, ky) != (0, 0)],
    key=lambda k: -(ring_hops(k[0], NX) + ring_hops(k[1], NY)),
)
LINE_STEPS = sorted(range(1, NZ), key=lambda k: -ring_hops(k, NZ))


def halves(value):
    high = value.astype(bf16)
    low = (value - high.astype(f32)).astype(bf16)
    return high, low


def dot(left, right, dims):
    return lax.dot_general(left, right, dims, preferred_element_type=f32)


def tile_at(i):
    return pl.ds(i * TILE if isinstance(i, int) else pl.multiple_of(i * TILE, TILE), TILE)


def kernel(
    counts, ids_in, samples_in, targets_in, inverse_in, out,
    ids, samples, targets, inverse,
    x_high, x_low, r_turned, residual, p_high, p_low, c_high, c_low, b_high, b_low,
    turned_high, turned_low, cross_high, cross_low,
    part, landing, line, line_in, full, swapped,
    in_sems, send_sems, recv_sems,
):
    z, x, y = (lax.axis_index(name) for name in ROWS)
    core = lax.axis_index("tgt")
    place = x * NY + y
    rows = samples.shape[0]
    tiles = rows // TILE
    blocks, block = ids.shape
    mine = block // 2
    unit = part.shape[1]
    piece = unit // PLANE
    wide = targets.shape[1]

    def plane_peer(step):
        px, py = lax.rem(x + step[0], NX), lax.rem(y + step[1], NY)
        return (z, px, py, core), px * NY + py

    def line_peer(step):
        return (lax.rem(z + step, NZ), x, y, core)

    partner = (z, x, y, 1 - core)

    barrier = pltpu.get_barrier_semaphore()
    for step in PLANE_STEPS:
        pl.semaphore_signal(barrier, inc=1, device_id=plane_peer(step)[0], device_id_type=MESH)
    for step in LINE_STEPS:
        pl.semaphore_signal(barrier, inc=1, device_id=line_peer(step), device_id_type=MESH)
    pl.semaphore_signal(barrier, inc=1, device_id=partner, device_id_type=MESH)

    chunk = rows // CHUNKS
    ids_copy = pltpu.make_async_copy(ids_in, ids, in_sems.at[CHUNKS])
    targets_copy = pltpu.make_async_copy(targets_in, targets, in_sems.at[CHUNKS + 1])
    inverse_copy = pltpu.make_async_copy(inverse_in, inverse, in_sems.at[CHUNKS + 2])

    def samples_copy(n):
        at = pl.ds(n * chunk, chunk)
        return pltpu.make_async_copy(samples_in.at[at], samples.at[at], in_sems.at[n])

    ids_copy.start()
    for n in range(CHUNKS):
        samples_copy(n).start()

    def remote(src, dst, stage, device):
        return pltpu.make_async_remote_copy(
            src_ref=src, dst_ref=dst, send_sem=send_sems.at[stage], recv_sem=recv_sems.at[stage],
            device_id=device, device_id_type=MESH,
        )

    def arrived(u, n, ref):
        pltpu.make_async_copy(ref, ref, recv_sems.at[4 * u + n]).wait()

    def sent(u, n, ref):
        pltpu.make_async_copy(ref, ref, send_sems.at[4 * u + n]).wait()

    own_piece = pl.ds(pl.multiple_of(place * piece, piece), piece)

    def scatter(u):
        for slot, step in enumerate(PLANE_STEPS):
            device, index = plane_peer(step)
            src = part.at[u, pl.ds(pl.multiple_of(index * piece, piece), piece)]
            remote(src, landing.at[u, slot], 4 * u, device).start()

    def to_line(u):
        arrived(u, 0, landing.at[u])
        total = part[u, own_piece]
        for slot in range(PLANE - 1):
            total = total + landing[u, slot]
        line[u] = total
        for slot, step in enumerate(LINE_STEPS):
            remote(line.at[u], line_in.at[u, slot], 4 * u + 1, line_peer(step)).start()

    def off_line(u):
        arrived(u, 1, line_in.at[u])
        total = line[u]
        for slot in range(NZ - 1):
            total = total + line_in[u, slot]
        return total

    def gather(u, value):
        full[u, own_piece] = value
        ref = full.at[u, own_piece]
        for step in PLANE_STEPS:
            remote(ref, ref, 4 * u + 2, plane_peer(step)[0]).start()

    def gathered(u):
        arrived(u, 2, landing.at[u])

    def swap(u):
        gathered(u)
        remote(full.at[u], swapped.at[u], 4 * u + 3, partner).start()

    per_chunk = tiles // CHUNKS
    for n in range(CHUNKS):
        samples_copy(n).wait()

        def split_samples(i, carry):
            at = tile_at(i)
            x_high[at], x_low[at] = halves(samples[at])
            return carry

        lax.fori_loop(n * per_chunk, (n + 1) * per_chunk, split_samples, 0)
    targets_copy.start()
    inverse_copy.start()
    ids_copy.wait()

    first = ((z * NX + x) * NY + y) * rows

    def pick(u):
        start = pl.multiple_of(core * mine + (u % 2) * unit, unit)
        wanted = ids[pl.ds(u // 2, 1), pl.ds(start, unit)] - first
        column = jnp.broadcast_to(wanted.astype(f32), (8, unit)).T[:, :1]
        slots = lax.broadcasted_iota(jnp.int32, (unit, rows), 1).astype(f32)
        chosen = jnp.where(column == slots, 1.0, 0.0).astype(bf16)
        part[u] = dot(chosen, x_high[...], NN) + dot(chosen, x_low[...], NN)

    pick(0)
    pl.semaphore_wait(barrier, PLANE + NZ - 1)
    scatter(0)
    pick(1)
    scatter(1)
    pick(2)
    pick(3)

    targets_copy.wait()

    def turn_targets(i, carry):
        at = tile_at(i)
        high, low = halves(targets[at].T)
        r_turned[pl.ds(0, wide), at] = high
        r_turned[pl.ds(wide, wide), at] = low
        return carry

    lax.fori_loop(0, tiles, turn_targets, 0)
    to_line(0)
    to_line(1)
    scatter(2)
    scatter(3)

    inverse_copy.wait()
    for b in range(blocks):
        for i in range(2):
            for j in range(2):
                from_i = pl.ds(pl.multiple_of((core + i) % 2 * mine, mine), mine)
                from_j = pl.ds(pl.multiple_of((core + j) % 2 * mine, mine), mine)
                high, low = halves(inverse[b, from_i, from_j])
                b_high[b, pl.ds(i * mine, mine), pl.ds(j * mine, mine)] = high
                b_low[b, pl.ds(i * mine, mine), pl.ds(j * mine, mine)] = low

    gather(0, off_line(0))
    gather(1, off_line(1))
    to_line(2)
    to_line(3)

    scale = 0.5 / samples.shape[1] ** 0.5

    def points_ready(b, h):
        for n in range(2):
            u = 2 * b + n
            if h == 1:
                arrived(u, 3, swapped.at[u])
            value = swapped[u] if h == 1 else full[u]
            at = pl.ds(h * mine + n * unit, unit)
            p_high[b, at], p_low[b, at] = halves(value * scale)

    live = counts[0]

    def columns(b, h, i):
        at, points = tile_at(i), pl.ds(h * mine, mine)
        high, low = p_high[b, points], p_low[b, points]
        near = (dot(x_high[at], high, NT) + dot(x_high[at], low, NT) + dot(x_low[at], high, NT)) + 1.0
        slots = i * TILE + lax.broadcasted_iota(jnp.int32, near.shape, 0)
        cubed = jnp.where(slots < live, near * near * near, 0.0)
        c_high[b, at, points], c_low[b, at, points] = halves(cubed)
        return cubed

    def sums(b, h):
        points = pl.ds(h * mine, mine)
        both = dot(r_turned[...], c_high[b, :, points], NN)
        value = both[:wide] + both[wide:] + dot(r_turned[pl.ds(0, wide)], c_low[b, :, points], NN)
        part[2 * (blocks + b) + h] = value

    def update(u, i, current):
        b, h = u // 2 - blocks, u % 2
        points = pl.ds(h * mine, mine)
        high, low = halves(full[u])
        both = dot(c_high[b, tile_at(i), points], jnp.concatenate([high, low], axis=0), NT)
        return current - (both[:, :wide] + both[:, wide:] + dot(c_low[b, tile_at(i), points], high, NT))

    def coefs(b):
        first_unit = 2 * (blocks + b)
        sums = jnp.concatenate([off_line(first_unit), off_line(first_unit + 1)], axis=1)
        high, low = halves(sums)
        both = jnp.concatenate([high, low], axis=0)
        for h in range(2):
            at = pl.ds(h * mine, mine)
            value = dot(both, b_high[b, at], NT)
            gather(first_unit + h, value[:piece] + value[piece:] + dot(high, b_low[b, at], NT))

    swap(0)
    swap(1)
    points_ready(0, 0)
    gather(2, off_line(2))
    gather(3, off_line(3))

    for h in range(2):
        if h == 1:
            points_ready(0, 1)
        for i in range(tiles):
            columns(0, h, i)
        sums(0, h)
        scatter(4 + h)

    swap(2)
    swap(3)
    for h in range(2):
        points_ready(1, h)
        for i in range(tiles):
            high, low = halves(columns(1, h, i).T)
            turned_high[pl.ds(h * mine, mine), tile_at(i)] = high
            turned_low[pl.ds(h * mine, mine), tile_at(i)] = low
    to_line(4)
    to_line(5)
    for h in range(2):
        at = pl.ds(h * mine, mine)
        sums(1, h)
        value = (
            dot(turned_high[at], c_high[0], NN)
            + dot(turned_high[at], c_low[0], NN)
            + dot(turned_low[at], c_high[0], NN)
        )
        cross_high[at], cross_low[at] = halves(value)
    coefs(0)

    gathered(4)
    gathered(5)
    high, low = halves(jnp.concatenate([full[4], full[5]], axis=1))
    both = jnp.concatenate([high, low], axis=0)
    for h in range(2):
        at = pl.ds(h * mine, mine)
        value = dot(both, cross_high[at], NT)
        part[6 + h] -= value[:wide] + value[wide:] + dot(high, cross_low[at], NT)
        scatter(6 + h)

    for i in range(tiles):
        at = tile_at(i)
        residual[at] = update(5, i, update(4, i, targets[at]))
    to_line(6)
    to_line(7)
    coefs(1)
    gathered(6)
    for i in range(tiles):
        at = tile_at(i)
        residual[at] = update(6, i, residual[at])
    gathered(7)
    for i in range(tiles):
        at = tile_at(i)
        out[at] = update(7, i, residual[at])

    for u in range(4 * blocks):
        sent(u, 0, landing.at[u])
        sent(u, 1, line_in.at[u])
        sent(u, 2, landing.at[u])
        if u < 2 * blocks:
            sent(u, 3, swapped.at[u])


def on_device(counts, samples, targets, point_ids, block_inverse):
    rows, feat = samples.shape
    blocks, block = point_ids.shape
    wide = targets.shape[1]
    units, unit, lanes = 4 * blocks, block // 4, block // 2
    piece = unit // PLANE
    anywhere = pl.BlockSpec(memory_space=pl.ANY)
    return pl.pallas_call(
        kernel,
        out_shape=pltpu.VMEM(targets.shape, f32),
        in_specs=[pl.BlockSpec(memory_space=pltpu.SMEM)] + [anywhere] * 4,
        out_specs=pl.BlockSpec(memory_space=pltpu.VMEM),
        scratch_shapes=[
            pltpu.VMEM(point_ids.shape, jnp.int32),
            pltpu.VMEM((rows, feat), f32),
            pltpu.VMEM((rows, wide), f32),
            pltpu.VMEM((blocks, block, block), f32),
            pltpu.VMEM((rows, feat), bf16),
            pltpu.VMEM((rows, feat), bf16),
            pltpu.VMEM((2 * wide, rows), bf16),
            pltpu.VMEM((rows, wide), f32),
            pltpu.VMEM((blocks, block, feat), bf16),
            pltpu.VMEM((blocks, block, feat), bf16),
            pltpu.VMEM((blocks, rows, block), bf16),
            pltpu.VMEM((blocks, rows, block), bf16),
            pltpu.VMEM((blocks, block, block), bf16),
            pltpu.VMEM((blocks, block, block), bf16),
            pltpu.VMEM((block, rows), bf16),
            pltpu.VMEM((block, rows), bf16),
            pltpu.VMEM((block, block), bf16),
            pltpu.VMEM((block, block), bf16),
            pltpu.VMEM((units, unit, lanes), f32),
            pltpu.VMEM((units, PLANE - 1, piece, lanes), f32),
            pltpu.VMEM((units, piece, lanes), f32),
            pltpu.VMEM((units, NZ - 1, piece, lanes), f32),
            pltpu.VMEM((units, unit, lanes), f32),
            pltpu.VMEM((2 * blocks, unit, lanes), f32),
            pltpu.SemaphoreType.DMA((CHUNKS + 3,)),
            pltpu.SemaphoreType.DMA((4 * units,)),
            pltpu.SemaphoreType.DMA((4 * units,)),
        ],
        compiler_params=pltpu.CompilerParams(collective_id=0, has_side_effects=True),
    )(counts, point_ids, samples, targets, block_inverse)


def solution(mesh):
    finer = Mesh(
        mesh.devices.reshape(NZ, NX, NY, mesh.shape["tgt"]), ("rows_0", "rows_1", "rows_2", "tgt")
    )
    placed = (P(ROWS), P(ROWS, None), P(ROWS, "tgt"), P(), P())
    return jax.shard_map(
        on_device, mesh=finer, in_specs=placed, out_specs=P(ROWS, "tgt"), check_vma=False
    )
```

```python
import jax
import jax.numpy as jnp
from jax import lax
from jax.experimental import pallas as pl
from jax.experimental.pallas import tpu as pltpu
from jax.sharding import Mesh
from jax.sharding import PartitionSpec as P

ROWS = ("rows_0", "rows_1", "rows_2")
MESH = pl.DeviceIdType.MESH
NZ, NX, NY = 8, 4, 4
PLANE = NX * NY
TILE = 256
CHUNKS = 4
NT = (((1,), (1,)), ((), ()))
NN = (((1,), (0,)), ((), ()))
f32, bf16 = jnp.float32, jnp.bfloat16


def ring_hops(step, size):
    return min(step, size - step)


PLANE_STEPS = sorted(
    [(kx, ky) for kx in range(NX) for ky in range(NY) if (kx, ky) != (0, 0)],
    key=lambda k: -(ring_hops(k[0], NX) + ring_hops(k[1], NY)),
)
LINE_STEPS = sorted(range(1, NZ), key=lambda k: -ring_hops(k, NZ))


def halves(value):
    high = value.astype(bf16)
    low = (value - high.astype(f32)).astype(bf16)
    return high, low


def dot(left, right, dims):
    return lax.dot_general(left, right, dims, preferred_element_type=f32)


def tile_at(i):
    return pl.ds(i * TILE if isinstance(i, int) else pl.multiple_of(i * TILE, TILE), TILE)


def kernel(
    counts_in, ids_in, samples_in, targets_in, inverse_in, out,
    counts, ids, samples, targets, inverse,
    x_high, x_low, r_turned, residual, p_high, p_low, c_high, c_low, b_high, b_low,
    turned_high, turned_low, cross_high, cross_low,
    part, landing, line, line_in, full, swapped,
    in_sems, send_sems, recv_sems,
):
    z, x, y = (lax.axis_index(name) for name in ROWS)
    core = lax.axis_index("tgt")
    place = x * NY + y
    rows = samples.shape[0]
    tiles = rows // TILE
    blocks, block = ids.shape
    mine = block // 2
    unit = part.shape[1]
    piece = unit // PLANE
    wide = targets.shape[1]

    def plane_peer(step):
        px, py = lax.rem(x + step[0], NX), lax.rem(y + step[1], NY)
        return (z, px, py, core), px * NY + py

    def line_peer(step):
        return (lax.rem(z + step, NZ), x, y, core)

    partner = (z, x, y, 1 - core)

    barrier = pltpu.get_barrier_semaphore()
    for step in LINE_STEPS:
        pl.semaphore_signal(barrier, inc=1, device_id=line_peer(step), device_id_type=MESH)
    for step in PLANE_STEPS:
        pl.semaphore_signal(barrier, inc=1, device_id=plane_peer(step)[0], device_id_type=MESH)
    pl.semaphore_signal(barrier, inc=1, device_id=partner, device_id_type=MESH)

    chunk = rows // CHUNKS
    counts_copy = pltpu.make_async_copy(counts_in, counts, in_sems.at[CHUNKS + 3])
    ids_copy = pltpu.make_async_copy(ids_in, ids, in_sems.at[CHUNKS])
    targets_copy = pltpu.make_async_copy(targets_in, targets, in_sems.at[CHUNKS + 1])
    inverse_copy = pltpu.make_async_copy(inverse_in, inverse, in_sems.at[CHUNKS + 2])

    def samples_copy(n):
        at = pl.ds(n * chunk, chunk)
        return pltpu.make_async_copy(samples_in.at[at], samples.at[at], in_sems.at[n])

    counts_copy.start()
    ids_copy.start()
    for n in range(CHUNKS):
        samples_copy(n).start()
    targets_copy.start()
    inverse_copy.start()

    def remote(src, dst, stage, device):
        return pltpu.make_async_remote_copy(
            src_ref=src, dst_ref=dst, send_sem=send_sems.at[stage], recv_sem=recv_sems.at[stage],
            device_id=device, device_id_type=MESH,
        )

    def arrived(u, n, ref):
        pltpu.make_async_copy(ref, ref, recv_sems.at[4 * u + n]).wait()

    def sent(u, n, ref):
        pltpu.make_async_copy(ref, ref, send_sems.at[4 * u + n]).wait()

    own_piece = pl.ds(pl.multiple_of(place * piece, piece), piece)

    def scatter(u):
        for slot, step in enumerate(PLANE_STEPS):
            device, index = plane_peer(step)
            src = part.at[u, pl.ds(pl.multiple_of(index * piece, piece), piece)]
            remote(src, landing.at[u, slot], 4 * u, device).start()

    def to_line(u):
        arrived(u, 0, landing.at[u])
        total = part[u, own_piece]
        for slot in range(PLANE - 1):
            total = total + landing[u, slot]
        line[u] = total
        for slot, step in enumerate(LINE_STEPS):
            remote(line.at[u], line_in.at[u, slot], 4 * u + 1, line_peer(step)).start()

    def off_line(u):
        arrived(u, 1, line_in.at[u])
        total = line[u]
        for slot in range(NZ - 1):
            total = total + line_in[u, slot]
        return total

    def gather(u, value):
        full[u, own_piece] = value
        ref = full.at[u, own_piece]
        for step in PLANE_STEPS:
            remote(ref, ref, 4 * u + 2, plane_peer(step)[0]).start()

    def gathered(u):
        arrived(u, 2, landing.at[u])

    def swap(u):
        gathered(u)
        remote(full.at[u], swapped.at[u], 4 * u + 3, partner).start()

    per_chunk = tiles // CHUNKS
    for n in range(CHUNKS):
        samples_copy(n).wait()

        def split_samples(i, carry):
            at = tile_at(i)
            x_high[at], x_low[at] = halves(samples[at])
            return carry

        lax.fori_loop(n * per_chunk, (n + 1) * per_chunk, split_samples, 0)
    ids_copy.wait()
    counts_copy.wait()

    first = ((z * NX + x) * NY + y) * rows

    def pick(u):
        start = pl.multiple_of(core * mine + (u % 2) * unit, unit)
        wanted = ids[pl.ds(u // 2, 1), pl.ds(start, unit)] - first
        column = jnp.broadcast_to(wanted.astype(f32), (8, unit)).T[:, :1]
        slots = lax.broadcasted_iota(jnp.int32, (unit, rows), 1).astype(f32)
        chosen = jnp.where(column == slots, 1.0, 0.0).astype(bf16)
        part[u] = dot(chosen, x_high[...], NN) + dot(chosen, x_low[...], NN)

    for u in range(2 * blocks):
        pick(u)
    pl.semaphore_wait(barrier, PLANE + NZ - 1)
    scatter(0)
    scatter(1)

    targets_copy.wait()

    def turn_targets(i, carry):
        at = tile_at(i)
        high, low = halves(targets[at].T)
        r_turned[pl.ds(0, wide), at] = high
        r_turned[pl.ds(wide, wide), at] = low
        return carry

    lax.fori_loop(0, tiles, turn_targets, 0)

    inverse_copy.wait()
    for b in range(blocks):
        for i in range(2):
            for j in range(2):
                from_i = pl.ds(pl.multiple_of((core + i) % 2 * mine, mine), mine)
                from_j = pl.ds(pl.multiple_of((core + j) % 2 * mine, mine), mine)
                high, low = halves(inverse[b, from_i, from_j])
                b_high[b, pl.ds(i * mine, mine), pl.ds(j * mine, mine)] = high
                b_low[b, pl.ds(i * mine, mine), pl.ds(j * mine, mine)] = low

    to_line(0)
    to_line(1)
    scatter(2)
    scatter(3)
    gather(0, off_line(0))
    gather(1, off_line(1))
    to_line(2)
    to_line(3)

    scale = 0.5 / samples.shape[1] ** 0.5

    def points_ready(b, h):
        for n in range(2):
            u = 2 * b + n
            if h == 1:
                arrived(u, 3, swapped.at[u])
            value = swapped[u] if h == 1 else full[u]
            at = pl.ds(h * mine + n * unit, unit)
            p_high[b, at], p_low[b, at] = halves(value * scale)

    live = counts[0]

    def columns(b, h, i):
        at, points = tile_at(i), pl.ds(h * mine, mine)
        high, low = p_high[b, points], p_low[b, points]
        near = (dot(x_high[at], high, NT) + dot(x_high[at], low, NT) + dot(x_low[at], high, NT)) + 1.0
        slots = i * TILE + lax.broadcasted_iota(jnp.int32, near.shape, 0)
        cubed = jnp.where(slots < live, near * near * near, 0.0)
        c_high[b, at, points], c_low[b, at, points] = halves(cubed)
        return cubed

    def sums(b, h):
        points = pl.ds(h * mine, mine)
        both = dot(r_turned[...], c_high[b, :, points], NN)
        value = both[:wide] + both[wide:] + dot(r_turned[pl.ds(0, wide)], c_low[b, :, points], NN)
        part[2 * (blocks + b) + h] = value

    def update(u, i, current):
        b, h = u // 2 - blocks, u % 2
        points = pl.ds(h * mine, mine)
        high, low = halves(full[u])
        both = dot(c_high[b, tile_at(i), points], jnp.concatenate([high, low], axis=0), NT)
        return current - (both[:, :wide] + both[:, wide:] + dot(c_low[b, tile_at(i), points], high, NT))

    def coefs(b):
        first_unit = 2 * (blocks + b)
        sums = jnp.concatenate([off_line(first_unit), off_line(first_unit + 1)], axis=1)
        high, low = halves(sums)
        both = jnp.concatenate([high, low], axis=0)
        for h in range(2):
            at = pl.ds(h * mine, mine)
            value = dot(both, b_high[b, at], NT)
            gather(first_unit + h, value[:piece] + value[piece:] + dot(high, b_low[b, at], NT))

    swap(0)
    swap(1)
    points_ready(0, 0)
    gather(2, off_line(2))
    gather(3, off_line(3))

    for h in range(2):
        if h == 1:
            points_ready(0, 1)
        for i in range(tiles):
            columns(0, h, i)
        sums(0, h)
        scatter(4 + h)

    swap(2)
    swap(3)
    for h in range(2):
        points_ready(1, h)
        for i in range(tiles):
            high, low = halves(columns(1, h, i).T)
            turned_high[pl.ds(h * mine, mine), tile_at(i)] = high
            turned_low[pl.ds(h * mine, mine), tile_at(i)] = low
    to_line(4)
    to_line(5)
    for h in range(2):
        at = pl.ds(h * mine, mine)
        sums(1, h)
        value = (
            dot(turned_high[at], c_high[0], NN)
            + dot(turned_high[at], c_low[0], NN)
            + dot(turned_low[at], c_high[0], NN)
        )
        cross_high[at], cross_low[at] = halves(value)
    coefs(0)

    gathered(4)
    gathered(5)
    high, low = halves(jnp.concatenate([full[4], full[5]], axis=1))
    both = jnp.concatenate([high, low], axis=0)
    for h in range(2):
        at = pl.ds(h * mine, mine)
        value = dot(both, cross_high[at], NT)
        part[6 + h] -= value[:wide] + value[wide:] + dot(high, cross_low[at], NT)
        scatter(6 + h)

    for i in range(tiles):
        at = tile_at(i)
        residual[at] = update(5, i, update(4, i, targets[at]))
    to_line(6)
    to_line(7)
    coefs(1)
    gathered(6)
    for i in range(tiles):
        at = tile_at(i)
        residual[at] = update(6, i, residual[at])
    gathered(7)
    for i in range(tiles):
        at = tile_at(i)
        out[at] = update(7, i, residual[at])

    for u in range(4 * blocks):
        sent(u, 0, landing.at[u])
        sent(u, 1, line_in.at[u])
        sent(u, 2, landing.at[u])
        if u < 2 * blocks:
            sent(u, 3, swapped.at[u])


def on_device(counts, samples, targets, point_ids, block_inverse):
    rows, feat = samples.shape
    blocks, block = point_ids.shape
    wide = targets.shape[1]
    units, unit, lanes = 4 * blocks, block // 4, block // 2
    piece = unit // PLANE
    anywhere = pl.BlockSpec(memory_space=pl.ANY)
    return pl.pallas_call(
        kernel,
        out_shape=pltpu.VMEM(targets.shape, f32),
        in_specs=[anywhere] * 5,
        out_specs=pl.BlockSpec(memory_space=pltpu.VMEM),
        scratch_shapes=[
            pltpu.SMEM(counts.shape, jnp.int32),
            pltpu.VMEM(point_ids.shape, jnp.int32),
            pltpu.VMEM((rows, feat), f32),
            pltpu.VMEM((rows, wide), f32),
            pltpu.VMEM((blocks, block, block), f32),
            pltpu.VMEM((rows, feat), bf16),
            pltpu.VMEM((rows, feat), bf16),
            pltpu.VMEM((2 * wide, rows), bf16),
            pltpu.VMEM((rows, wide), f32),
            pltpu.VMEM((blocks, block, feat), bf16),
            pltpu.VMEM((blocks, block, feat), bf16),
            pltpu.VMEM((blocks, rows, block), bf16),
            pltpu.VMEM((blocks, rows, block), bf16),
            pltpu.VMEM((blocks, block, block), bf16),
            pltpu.VMEM((blocks, block, block), bf16),
            pltpu.VMEM((block, rows), bf16),
            pltpu.VMEM((block, rows), bf16),
            pltpu.VMEM((block, block), bf16),
            pltpu.VMEM((block, block), bf16),
            pltpu.VMEM((units, unit, lanes), f32),
            pltpu.VMEM((units, PLANE - 1, piece, lanes), f32),
            pltpu.VMEM((units, piece, lanes), f32),
            pltpu.VMEM((units, NZ - 1, piece, lanes), f32),
            pltpu.VMEM((units, unit, lanes), f32),
            pltpu.VMEM((2 * blocks, unit, lanes), f32),
            pltpu.SemaphoreType.DMA((CHUNKS + 4,)),
            pltpu.SemaphoreType.DMA((4 * units,)),
            pltpu.SemaphoreType.DMA((4 * units,)),
        ],
        compiler_params=pltpu.CompilerParams(collective_id=0, has_side_effects=True),
    )(counts, point_ids, samples, targets, block_inverse)


def solution(mesh):
    finer = Mesh(
        mesh.devices.reshape(NZ, NX, NY, mesh.shape["tgt"]), ("rows_0", "rows_1", "rows_2", "tgt")
    )
    placed = (P(ROWS), P(ROWS, None), P(ROWS, "tgt"), P(), P())
    return jax.shard_map(
        on_device, mesh=finer, in_specs=placed, out_specs=P(ROWS, "tgt"), check_vma=False
    )
```

```python
import jax
import jax.numpy as jnp
from jax import lax
from jax.experimental import pallas as pl
from jax.experimental.pallas import tpu as pltpu
from jax.sharding import Mesh
from jax.sharding import PartitionSpec as P

ROWS = ("rows_0", "rows_1", "rows_2")
MESH = pl.DeviceIdType.MESH
NZ, NX, NY = 8, 4, 4
PLANE = NX * NY
TILE = 256
CHUNKS = 4
NT = (((1,), (1,)), ((), ()))
NN = (((1,), (0,)), ((), ()))
f32, bf16 = jnp.float32, jnp.bfloat16


def ring_hops(step, size):
    return min(step, size - step)


PLANE_STEPS = sorted(
    [(kx, ky) for kx in range(NX) for ky in range(NY) if (kx, ky) != (0, 0)],
    key=lambda k: -(ring_hops(k[0], NX) + ring_hops(k[1], NY)),
)
LINE_STEPS = sorted(range(1, NZ), key=lambda k: -ring_hops(k, NZ))


def halves(value):
    high = value.astype(bf16)
    low = (value - high.astype(f32)).astype(bf16)
    return high, low


def dot(left, right, dims):
    return lax.dot_general(left, right, dims, preferred_element_type=f32)


def tile_at(i):
    return pl.ds(i * TILE if isinstance(i, int) else pl.multiple_of(i * TILE, TILE), TILE)


def kernel(
    counts_in, ids_in, samples_in, targets_in, inverse_in, out,
    counts, ids, samples, targets, inverse,
    x_high, x_low, r_turned, residual, p_high, p_low, c_high, c_low, b_high, b_low,
    turned_high, turned_low, cross_high, cross_low,
    part, landing, line, line_in, full, swapped,
    in_sems, send_sems, recv_sems,
):
    z, x, y = (lax.axis_index(name) for name in ROWS)
    core = lax.axis_index("tgt")
    place = x * NY + y
    rows = samples.shape[0]
    tiles = rows // TILE
    blocks, block = ids.shape
    mine = block // 2
    unit = part.shape[1]
    piece = unit // PLANE
    wide = targets.shape[1]

    def plane_peer(step):
        px, py = lax.rem(x + step[0], NX), lax.rem(y + step[1], NY)
        return (z, px, py, core), px * NY + py

    def line_peer(step):
        return (lax.rem(z + step, NZ), x, y, core)

    partner = (z, x, y, 1 - core)

    barrier = pltpu.get_barrier_semaphore()
    for step in LINE_STEPS:
        pl.semaphore_signal(barrier, inc=1, device_id=line_peer(step), device_id_type=MESH)
    for step in PLANE_STEPS:
        pl.semaphore_signal(barrier, inc=1, device_id=plane_peer(step)[0], device_id_type=MESH)
    pl.semaphore_signal(barrier, inc=1, device_id=partner, device_id_type=MESH)

    chunk = rows // CHUNKS
    counts_copy = pltpu.make_async_copy(counts_in, counts, in_sems.at[CHUNKS + 3])
    ids_copy = pltpu.make_async_copy(ids_in, ids, in_sems.at[CHUNKS])
    targets_copy = pltpu.make_async_copy(targets_in, targets, in_sems.at[CHUNKS + 1])
    inverse_copy = pltpu.make_async_copy(inverse_in, inverse, in_sems.at[CHUNKS + 2])

    def samples_copy(n):
        at = pl.ds(n * chunk, chunk)
        return pltpu.make_async_copy(samples_in.at[at], samples.at[at], in_sems.at[n])

    counts_copy.start()
    ids_copy.start()
    for n in range(CHUNKS):
        samples_copy(n).start()
    targets_copy.start()
    inverse_copy.start()

    def remote(src, dst, stage, device):
        return pltpu.make_async_remote_copy(
            src_ref=src, dst_ref=dst, send_sem=send_sems.at[stage], recv_sem=recv_sems.at[stage],
            device_id=device, device_id_type=MESH,
        )

    def arrived(u, n, ref):
        pltpu.make_async_copy(ref, ref, recv_sems.at[4 * u + n]).wait()

    def sent(u, n, ref):
        pltpu.make_async_copy(ref, ref, send_sems.at[4 * u + n]).wait()

    own_piece = pl.ds(pl.multiple_of(place * piece, piece), piece)

    def scatter(u):
        for slot, step in enumerate(PLANE_STEPS):
            device, index = plane_peer(step)
            src = part.at[u, pl.ds(pl.multiple_of(index * piece, piece), piece)]
            remote(src, landing.at[u, slot], 4 * u, device).start()

    def to_line(u):
        arrived(u, 0, landing.at[u])
        total = part[u, own_piece]
        for slot in range(PLANE - 1):
            total = total + landing[u, slot]
        line[u] = total
        for slot, step in enumerate(LINE_STEPS):
            remote(line.at[u], line_in.at[u, slot], 4 * u + 1, line_peer(step)).start()

    def off_line(u):
        arrived(u, 1, line_in.at[u])
        total = line[u]
        for slot in range(NZ - 1):
            total = total + line_in[u, slot]
        return total

    def gather(u, value):
        full[u, own_piece] = value
        ref = full.at[u, own_piece]
        for step in PLANE_STEPS:
            remote(ref, ref, 4 * u + 2, plane_peer(step)[0]).start()

    def gathered(u):
        arrived(u, 2, landing.at[u])

    def swap(u):
        gathered(u)
        remote(full.at[u], swapped.at[u], 4 * u + 3, partner).start()

    per_chunk = tiles // CHUNKS
    for n in range(CHUNKS):
        samples_copy(n).wait()

        def split_samples(i, carry):
            at = tile_at(i)
            x_high[at], x_low[at] = halves(samples[at])
            return carry

        lax.fori_loop(n * per_chunk, (n + 1) * per_chunk, split_samples, 0)
    ids_copy.wait()
    counts_copy.wait()

    first = ((z * NX + x) * NY + y) * rows

    def pick(b):
        wanted = ids[pl.ds(b, 1), pl.ds(pl.multiple_of(core * mine, mine), mine)] - first
        column = jnp.broadcast_to(wanted.astype(f32), (8, mine)).T[:, :1]
        slots = lax.broadcasted_iota(jnp.int32, (mine, rows), 1).astype(f32)
        chosen = jnp.where(column == slots, 1.0, 0.0).astype(bf16)
        value = dot(chosen, x_high[...], NN) + dot(chosen, x_low[...], NN)
        for n in range(2):
            part[2 * b + n] = value[n * unit:(n + 1) * unit]

    pick(0)
    pl.semaphore_wait(barrier, PLANE + NZ - 1)
    scatter(0)
    scatter(1)
    pick(1)

    targets_copy.wait()

    def turn_targets(i, carry):
        at = tile_at(i)
        high, low = halves(targets[at].T)
        r_turned[pl.ds(0, wide), at] = high
        r_turned[pl.ds(wide, wide), at] = low
        return carry

    lax.fori_loop(0, tiles, turn_targets, 0)

    inverse_copy.wait()
    for b in range(blocks):
        for i in range(2):
            for j in range(2):
                from_i = pl.ds(pl.multiple_of((core + i) % 2 * mine, mine), mine)
                from_j = pl.ds(pl.multiple_of((core + j) % 2 * mine, mine), mine)
                high, low = halves(inverse[b, from_i, from_j])
                b_high[b, pl.ds(i * mine, mine), pl.ds(j * mine, mine)] = high
                b_low[b, pl.ds(i * mine, mine), pl.ds(j * mine, mine)] = low

    to_line(0)
    to_line(1)
    scatter(2)
    scatter(3)
    gather(0, off_line(0))
    gather(1, off_line(1))
    to_line(2)
    to_line(3)

    scale = 0.5 / samples.shape[1] ** 0.5

    def points_ready(b, h):
        for n in range(2):
            u = 2 * b + n
            if h == 1:
                arrived(u, 3, swapped.at[u])
            value = swapped[u] if h == 1 else full[u]
            at = pl.ds(h * mine + n * unit, unit)
            p_high[b, at], p_low[b, at] = halves(value * scale)

    live = counts[0]

    def columns(b, h, i):
        at, points = tile_at(i), pl.ds(h * mine, mine)
        high, low = p_high[b, points], p_low[b, points]
        near = (dot(x_high[at], high, NT) + dot(x_high[at], low, NT) + dot(x_low[at], high, NT)) + 1.0
        slots = i * TILE + lax.broadcasted_iota(jnp.int32, near.shape, 0)
        cubed = jnp.where(slots < live, near * near * near, 0.0)
        c_high[b, at, points], c_low[b, at, points] = halves(cubed)
        return cubed

    def sums(b, h):
        points = pl.ds(h * mine, mine)
        both = dot(r_turned[...], c_high[b, :, points], NN)
        value = both[:wide] + both[wide:] + dot(r_turned[pl.ds(0, wide)], c_low[b, :, points], NN)
        part[2 * (blocks + b) + h] = value

    def update(u, i, current):
        b, h = u // 2 - blocks, u % 2
        points = pl.ds(h * mine, mine)
        high, low = halves(full[u])
        both = dot(c_high[b, tile_at(i), points], jnp.concatenate([high, low], axis=0), NT)
        return current - (both[:, :wide] + both[:, wide:] + dot(c_low[b, tile_at(i), points], high, NT))

    def coefs(b):
        first_unit = 2 * (blocks + b)
        sums = jnp.concatenate([off_line(first_unit), off_line(first_unit + 1)], axis=1)
        high, low = halves(sums)
        both = jnp.concatenate([high, low], axis=0)
        for h in range(2):
            at = pl.ds(h * mine, mine)
            value = dot(both, b_high[b, at], NT)
            gather(first_unit + h, value[:piece] + value[piece:] + dot(high, b_low[b, at], NT))

    swap(0)
    swap(1)
    points_ready(0, 0)
    gather(2, off_line(2))
    gather(3, off_line(3))

    for h in range(2):
        if h == 1:
            points_ready(0, 1)
        for i in range(tiles):
            columns(0, h, i)
        sums(0, h)
        scatter(4 + h)

    def second_columns(h):
        points_ready(1, h)
        for i in range(tiles):
            high, low = halves(columns(1, h, i).T)
            turned_high[pl.ds(h * mine, mine), tile_at(i)] = high
            turned_low[pl.ds(h * mine, mine), tile_at(i)] = low

    def cross(h):
        at = pl.ds(h * mine, mine)
        value = (
            dot(turned_high[at], c_high[0], NN)
            + dot(turned_high[at], c_low[0], NN)
            + dot(turned_low[at], c_high[0], NN)
        )
        cross_high[at], cross_low[at] = halves(value)

    swap(2)
    swap(3)
    second_columns(0)
    to_line(4)
    to_line(5)
    second_columns(1)
    sums(1, 0)
    sums(1, 1)
    cross(0)
    coefs(0)
    cross(1)

    gathered(4)
    gathered(5)
    high, low = halves(jnp.concatenate([full[4], full[5]], axis=1))
    both = jnp.concatenate([high, low], axis=0)
    for h in range(2):
        at = pl.ds(h * mine, mine)
        value = dot(both, cross_high[at], NT)
        part[6 + h] -= value[:wide] + value[wide:] + dot(high, cross_low[at], NT)
        scatter(6 + h)

    for i in range(tiles):
        at = tile_at(i)
        residual[at] = update(5, i, update(4, i, targets[at]))
    to_line(6)
    to_line(7)
    coefs(1)
    gathered(6)
    for i in range(tiles):
        at = tile_at(i)
        residual[at] = update(6, i, residual[at])
    gathered(7)
    for i in range(tiles):
        at = tile_at(i)
        out[at] = update(7, i, residual[at])

    for u in range(4 * blocks):
        sent(u, 0, landing.at[u])
        sent(u, 1, line_in.at[u])
        sent(u, 2, landing.at[u])
        if u < 2 * blocks:
            sent(u, 3, swapped.at[u])


def on_device(counts, samples, targets, point_ids, block_inverse):
    rows, feat = samples.shape
    blocks, block = point_ids.shape
    wide = targets.shape[1]
    units, unit, lanes = 4 * blocks, block // 4, block // 2
    piece = unit // PLANE
    anywhere = pl.BlockSpec(memory_space=pl.ANY)
    return pl.pallas_call(
        kernel,
        out_shape=pltpu.VMEM(targets.shape, f32),
        in_specs=[anywhere] * 5,
        out_specs=pl.BlockSpec(memory_space=pltpu.VMEM),
        scratch_shapes=[
            pltpu.SMEM(counts.shape, jnp.int32),
            pltpu.VMEM(point_ids.shape, jnp.int32),
            pltpu.VMEM((rows, feat), f32),
            pltpu.VMEM((rows, wide), f32),
            pltpu.VMEM((blocks, block, block), f32),
            pltpu.VMEM((rows, feat), bf16),
            pltpu.VMEM((rows, feat), bf16),
            pltpu.VMEM((2 * wide, rows), bf16),
            pltpu.VMEM((rows, wide), f32),
            pltpu.VMEM((blocks, block, feat), bf16),
            pltpu.VMEM((blocks, block, feat), bf16),
            pltpu.VMEM((blocks, rows, block), bf16),
            pltpu.VMEM((blocks, rows, block), bf16),
            pltpu.VMEM((blocks, block, block), bf16),
            pltpu.VMEM((blocks, block, block), bf16),
            pltpu.VMEM((block, rows), bf16),
            pltpu.VMEM((block, rows), bf16),
            pltpu.VMEM((block, block), bf16),
            pltpu.VMEM((block, block), bf16),
            pltpu.VMEM((units, unit, lanes), f32),
            pltpu.VMEM((units, PLANE - 1, piece, lanes), f32),
            pltpu.VMEM((units, piece, lanes), f32),
            pltpu.VMEM((units, NZ - 1, piece, lanes), f32),
            pltpu.VMEM((units, unit, lanes), f32),
            pltpu.VMEM((2 * blocks, unit, lanes), f32),
            pltpu.SemaphoreType.DMA((CHUNKS + 4,)),
            pltpu.SemaphoreType.DMA((4 * units,)),
            pltpu.SemaphoreType.DMA((4 * units,)),
        ],
        compiler_params=pltpu.CompilerParams(collective_id=0, has_side_effects=True),
    )(counts, point_ids, samples, targets, block_inverse)


def solution(mesh):
    finer = Mesh(
        mesh.devices.reshape(NZ, NX, NY, mesh.shape["tgt"]), ("rows_0", "rows_1", "rows_2", "tgt")
    )
    placed = (P(ROWS), P(ROWS, None), P(ROWS, "tgt"), P(), P())
    return jax.shard_map(
        on_device, mesh=finer, in_specs=placed, out_specs=P(ROWS, "tgt"), check_vma=False
    )
```

```python
import jax
import jax.numpy as jnp
from jax import lax
from jax.experimental import pallas as pl
from jax.experimental.pallas import tpu as pltpu
from jax.sharding import Mesh
from jax.sharding import PartitionSpec as P

ROWS = ("rows_0", "rows_1", "rows_2")
MESH = pl.DeviceIdType.MESH
NZ, NX, NY = 8, 4, 4
PLANE = NX * NY
TILE = 256
CHUNKS = 4
NT = (((1,), (1,)), ((), ()))
NN = (((1,), (0,)), ((), ()))
f32, bf16 = jnp.float32, jnp.bfloat16


def ring_hops(step, size):
    return min(step, size - step)


PLANE_STEPS = sorted(
    [(kx, ky) for kx in range(NX) for ky in range(NY) if (kx, ky) != (0, 0)],
    key=lambda k: -(ring_hops(k[0], NX) + ring_hops(k[1], NY)),
)
LINE_STEPS = sorted(range(1, NZ), key=lambda k: -ring_hops(k, NZ))


def halves(value):
    high = value.astype(bf16)
    low = (value - high.astype(f32)).astype(bf16)
    return high, low


def dot(left, right, dims):
    return lax.dot_general(left, right, dims, preferred_element_type=f32)


def tile_at(i):
    return pl.ds(i * TILE if isinstance(i, int) else pl.multiple_of(i * TILE, TILE), TILE)


def kernel(
    counts_in, ids_in, samples_in, targets_in, inverse_in, out,
    counts, ids, samples, targets, inverse,
    x_high, x_low, r_turned, residual, p_high, p_low, c_high, c_low, b_high, b_low,
    turned_high, turned_low, cross_high, cross_low, solved_high, solved_low,
    part, landing, line, line_in, full, swapped,
    in_sems, send_sems, recv_sems,
):
    z, x, y = (lax.axis_index(name) for name in ROWS)
    core = lax.axis_index("tgt")
    place = x * NY + y
    rows = samples.shape[0]
    tiles = rows // TILE
    blocks, block = ids.shape
    mine = block // 2
    unit = part.shape[1]
    piece = unit // PLANE
    wide = targets.shape[1]

    def plane_peer(step):
        px, py = lax.rem(x + step[0], NX), lax.rem(y + step[1], NY)
        return (z, px, py, core), px * NY + py

    def line_peer(step):
        return (lax.rem(z + step, NZ), x, y, core)

    partner = (z, x, y, 1 - core)

    barrier = pltpu.get_barrier_semaphore()
    for step in LINE_STEPS:
        pl.semaphore_signal(barrier, inc=1, device_id=line_peer(step), device_id_type=MESH)
    for step in PLANE_STEPS:
        pl.semaphore_signal(barrier, inc=1, device_id=plane_peer(step)[0], device_id_type=MESH)
    pl.semaphore_signal(barrier, inc=1, device_id=partner, device_id_type=MESH)

    chunk = rows // CHUNKS
    counts_copy = pltpu.make_async_copy(counts_in, counts, in_sems.at[CHUNKS + 3])
    ids_copy = pltpu.make_async_copy(ids_in, ids, in_sems.at[CHUNKS])
    targets_copy = pltpu.make_async_copy(targets_in, targets, in_sems.at[CHUNKS + 1])
    inverse_copy = pltpu.make_async_copy(inverse_in, inverse, in_sems.at[CHUNKS + 2])

    def samples_copy(n):
        at = pl.ds(n * chunk, chunk)
        return pltpu.make_async_copy(samples_in.at[at], samples.at[at], in_sems.at[n])

    counts_copy.start()
    ids_copy.start()
    for n in range(CHUNKS):
        samples_copy(n).start()
    targets_copy.start()
    inverse_copy.start()

    def remote(src, dst, stage, device):
        return pltpu.make_async_remote_copy(
            src_ref=src, dst_ref=dst, send_sem=send_sems.at[stage], recv_sem=recv_sems.at[stage],
            device_id=device, device_id_type=MESH,
        )

    def arrived(u, n, ref):
        pltpu.make_async_copy(ref, ref, recv_sems.at[4 * u + n]).wait()

    def sent(u, n, ref):
        pltpu.make_async_copy(ref, ref, send_sems.at[4 * u + n]).wait()

    own_piece = pl.ds(pl.multiple_of(place * piece, piece), piece)

    def scatter(u):
        for slot, step in enumerate(PLANE_STEPS):
            device, index = plane_peer(step)
            src = part.at[u, pl.ds(pl.multiple_of(index * piece, piece), piece)]
            remote(src, landing.at[u, slot], 4 * u, device).start()

    def to_line(u):
        arrived(u, 0, landing.at[u])
        total = part[u, own_piece]
        for slot in range(PLANE - 1):
            total = total + landing[u, slot]
        line[u] = total
        for slot, step in enumerate(LINE_STEPS):
            remote(line.at[u], line_in.at[u, slot], 4 * u + 1, line_peer(step)).start()

    def off_line(u):
        arrived(u, 1, line_in.at[u])
        total = line[u]
        for slot in range(NZ - 1):
            total = total + line_in[u, slot]
        return total

    def gather(u, value):
        full[u, own_piece] = value
        ref = full.at[u, own_piece]
        for step in PLANE_STEPS:
            remote(ref, ref, 4 * u + 2, plane_peer(step)[0]).start()

    def gathered(u):
        arrived(u, 2, landing.at[u])

    def swap(u):
        gathered(u)
        remote(full.at[u], swapped.at[u], 4 * u + 3, partner).start()

    per_chunk = tiles // CHUNKS
    for n in range(CHUNKS):
        samples_copy(n).wait()

        def split_samples(i, carry):
            at = tile_at(i)
            x_high[at], x_low[at] = halves(samples[at])
            return carry

        lax.fori_loop(n * per_chunk, (n + 1) * per_chunk, split_samples, 0)
    ids_copy.wait()
    counts_copy.wait()

    first = ((z * NX + x) * NY + y) * rows

    def pick(b):
        wanted = ids[pl.ds(b, 1), pl.ds(pl.multiple_of(core * mine, mine), mine)] - first
        column = jnp.broadcast_to(wanted.astype(f32), (8, mine)).T[:, :1]
        slots = lax.broadcasted_iota(jnp.int32, (mine, rows), 1).astype(f32)
        chosen = jnp.where(column == slots, 1.0, 0.0).astype(bf16)
        value = dot(chosen, x_high[...], NN) + dot(chosen, x_low[...], NN)
        for n in range(2):
            part[2 * b + n] = value[n * unit:(n + 1) * unit]

    pick(0)
    pl.semaphore_wait(barrier, PLANE + NZ - 1)
    scatter(0)
    scatter(1)
    pick(1)

    targets_copy.wait()

    def turn_targets(i, carry):
        at = tile_at(i)
        high, low = halves(targets[at].T)
        r_turned[pl.ds(0, wide), at] = high
        r_turned[pl.ds(wide, wide), at] = low
        return carry

    lax.fori_loop(0, tiles, turn_targets, 0)

    inverse_copy.wait()
    for b in range(blocks):
        for i in range(2):
            for j in range(2):
                from_i = pl.ds(pl.multiple_of((core + i) % 2 * mine, mine), mine)
                from_j = pl.ds(pl.multiple_of((core + j) % 2 * mine, mine), mine)
                high, low = halves(inverse[b, from_i, from_j])
                b_high[b, pl.ds(i * mine, mine), pl.ds(j * mine, mine)] = high
                b_low[b, pl.ds(i * mine, mine), pl.ds(j * mine, mine)] = low

    to_line(0)
    to_line(1)
    scatter(2)
    scatter(3)
    gather(0, off_line(0))
    gather(1, off_line(1))
    to_line(2)
    to_line(3)

    scale = 0.5 / samples.shape[1] ** 0.5

    def points_ready(b, h):
        for n in range(2):
            u = 2 * b + n
            if h == 1:
                arrived(u, 3, swapped.at[u])
            value = swapped[u] if h == 1 else full[u]
            at = pl.ds(h * mine + n * unit, unit)
            p_high[b, at], p_low[b, at] = halves(value * scale)

    live = counts[0]

    def columns(b, h, i):
        at, points = tile_at(i), pl.ds(h * mine, mine)
        high, low = p_high[b, points], p_low[b, points]
        near = (dot(x_high[at], high, NT) + dot(x_high[at], low, NT) + dot(x_low[at], high, NT)) + 1.0
        slots = i * TILE + lax.broadcasted_iota(jnp.int32, near.shape, 0)
        cubed = jnp.where(slots < live, near * near * near, 0.0)
        c_high[b, at, points], c_low[b, at, points] = halves(cubed)
        return cubed

    def sums(b, h):
        points = pl.ds(h * mine, mine)
        both = dot(r_turned[...], c_high[b, :, points], NN)
        value = both[:wide] + both[wide:] + dot(r_turned[pl.ds(0, wide)], c_low[b, :, points], NN)
        part[2 * (blocks + b) + h] = value

    def update(u, i, current):
        b, h = u // 2 - blocks, u % 2
        points = pl.ds(h * mine, mine)
        high, low = halves(full[u])
        both = dot(c_high[b, tile_at(i), points], jnp.concatenate([high, low], axis=0), NT)
        return current - (both[:, :wide] + both[:, wide:] + dot(c_low[b, tile_at(i), points], high, NT))

    def coefs():
        sums = jnp.concatenate([off_line(4), off_line(5)], axis=1)
        high, low = halves(sums)
        both = jnp.concatenate([high, low], axis=0)
        for h in range(2):
            at = pl.ds(h * mine, mine)
            value = dot(both, b_high[0, at], NT)
            gather(4 + h, value[:piece] + value[piece:] + dot(high, b_low[0, at], NT))

    swap(0)
    swap(1)
    points_ready(0, 0)
    gather(2, off_line(2))
    gather(3, off_line(3))

    for h in range(2):
        if h == 1:
            points_ready(0, 1)
        for i in range(tiles):
            columns(0, h, i)
        sums(0, h)
        scatter(4 + h)

    def second_columns(h):
        points_ready(1, h)
        for i in range(tiles):
            high, low = halves(columns(1, h, i).T)
            turned_high[pl.ds(h * mine, mine), tile_at(i)] = high
            turned_low[pl.ds(h * mine, mine), tile_at(i)] = low

    def cross(h):
        at = pl.ds(h * mine, mine)
        value = (
            dot(turned_high[at], c_high[0], NN)
            + dot(turned_high[at], c_low[0], NN)
            + dot(turned_low[at], c_high[0], NN)
        )
        cross_high[at], cross_low[at] = halves(value)

    swap(2)
    swap(3)
    second_columns(0)
    second_columns(1)
    to_line(4)
    to_line(5)
    sums(1, 0)
    sums(1, 1)
    cross(0)
    cross(1)
    coefs()

    early_high, early_low = halves(jnp.concatenate([part[6], part[7]], axis=1))
    for h in range(2):
        at = pl.ds(h * mine, mine)
        solved_high[at], solved_low[at] = halves(
            dot(b_high[1, at], cross_high[...], NN)
            + dot(b_high[1, at], cross_low[...], NN)
            + dot(b_low[1, at], cross_high[...], NN)
        )
        part[6 + h] = (
            dot(early_high, b_high[1, at], NT) + dot(early_high, b_low[1, at], NT) + dot(early_low, b_high[1, at], NT)
        )

    gathered(4)
    gathered(5)
    high, low = halves(jnp.concatenate([full[4], full[5]], axis=1))
    both = jnp.concatenate([high, low], axis=0)
    for h in range(2):
        at = pl.ds(h * mine, mine)
        value = dot(both, solved_high[at], NT)
        part[6 + h] -= value[:wide] + value[wide:] + dot(high, solved_low[at], NT)
        scatter(6 + h)

    for i in range(tiles):
        at = tile_at(i)
        residual[at] = update(5, i, update(4, i, targets[at]))
    to_line(6)
    to_line(7)
    gather(6, off_line(6))
    gather(7, off_line(7))
    gathered(6)
    for i in range(tiles):
        at = tile_at(i)
        residual[at] = update(6, i, residual[at])
    gathered(7)
    for i in range(tiles):
        at = tile_at(i)
        out[at] = update(7, i, residual[at])

    for u in range(4 * blocks):
        sent(u, 0, landing.at[u])
        sent(u, 1, line_in.at[u])
        sent(u, 2, landing.at[u])
        if u < 2 * blocks:
            sent(u, 3, swapped.at[u])


def on_device(counts, samples, targets, point_ids, block_inverse):
    rows, feat = samples.shape
    blocks, block = point_ids.shape
    wide = targets.shape[1]
    units, unit, lanes = 4 * blocks, block // 4, block // 2
    piece = unit // PLANE
    anywhere = pl.BlockSpec(memory_space=pl.ANY)
    return pl.pallas_call(
        kernel,
        out_shape=pltpu.VMEM(targets.shape, f32),
        in_specs=[anywhere] * 5,
        out_specs=pl.BlockSpec(memory_space=pltpu.VMEM),
        scratch_shapes=[
            pltpu.SMEM(counts.shape, jnp.int32),
            pltpu.VMEM(point_ids.shape, jnp.int32),
            pltpu.VMEM((rows, feat), f32),
            pltpu.VMEM((rows, wide), f32),
            pltpu.VMEM((blocks, block, block), f32),
            pltpu.VMEM((rows, feat), bf16),
            pltpu.VMEM((rows, feat), bf16),
            pltpu.VMEM((2 * wide, rows), bf16),
            pltpu.VMEM((rows, wide), f32),
            pltpu.VMEM((blocks, block, feat), bf16),
            pltpu.VMEM((blocks, block, feat), bf16),
            pltpu.VMEM((blocks, rows, block), bf16),
            pltpu.VMEM((blocks, rows, block), bf16),
            pltpu.VMEM((blocks, block, block), bf16),
            pltpu.VMEM((blocks, block, block), bf16),
            pltpu.VMEM((block, rows), bf16),
            pltpu.VMEM((block, rows), bf16),
            pltpu.VMEM((block, block), bf16),
            pltpu.VMEM((block, block), bf16),
            pltpu.VMEM((block, block), bf16),
            pltpu.VMEM((block, block), bf16),
            pltpu.VMEM((units, unit, lanes), f32),
            pltpu.VMEM((units, PLANE - 1, piece, lanes), f32),
            pltpu.VMEM((units, piece, lanes), f32),
            pltpu.VMEM((units, NZ - 1, piece, lanes), f32),
            pltpu.VMEM((units, unit, lanes), f32),
            pltpu.VMEM((2 * blocks, unit, lanes), f32),
            pltpu.SemaphoreType.DMA((CHUNKS + 4,)),
            pltpu.SemaphoreType.DMA((4 * units,)),
            pltpu.SemaphoreType.DMA((4 * units,)),
        ],
        compiler_params=pltpu.CompilerParams(collective_id=0, has_side_effects=True),
    )(counts, point_ids, samples, targets, block_inverse)


def solution(mesh):
    finer = Mesh(
        mesh.devices.reshape(NZ, NX, NY, mesh.shape["tgt"]), ("rows_0", "rows_1", "rows_2", "tgt")
    )
    placed = (P(ROWS), P(ROWS, None), P(ROWS, "tgt"), P(), P())
    return jax.shard_map(
        on_device, mesh=finer, in_specs=placed, out_specs=P(ROWS, "tgt"), check_vma=False
    )
```

```python
import jax
import jax.numpy as jnp
from jax import lax
from jax.experimental import pallas as pl
from jax.experimental.pallas import tpu as pltpu
from jax.sharding import Mesh
from jax.sharding import PartitionSpec as P

ROWS = ("rows_0", "rows_1", "rows_2")
MESH = pl.DeviceIdType.MESH
NZ, NX, NY = 8, 4, 4
PLANE = NX * NY
TILE = 256
CHUNKS = 4
NT = (((1,), (1,)), ((), ()))
NN = (((1,), (0,)), ((), ()))
f32, bf16 = jnp.float32, jnp.bfloat16


def ring_hops(step, size):
    return min(step, size - step)


PLANE_STEPS = sorted(
    [(kx, ky) for kx in range(NX) for ky in range(NY) if (kx, ky) != (0, 0)],
    key=lambda k: -(ring_hops(k[0], NX) + ring_hops(k[1], NY)),
)
LINE_STEPS = sorted(range(1, NZ), key=lambda k: -ring_hops(k, NZ))


def halves(value):
    high = value.astype(bf16)
    low = (value - high.astype(f32)).astype(bf16)
    return high, low


def dot(left, right, dims):
    return lax.dot_general(left, right, dims, preferred_element_type=f32)


def tile_at(i):
    return pl.ds(i * TILE if isinstance(i, int) else pl.multiple_of(i * TILE, TILE), TILE)


def kernel(
    counts_in, ids_in, samples_in, targets_in, inverse_in, out,
    counts, ids, samples, targets, inverse,
    x_high, x_low, r_turned, residual, p_high, p_low, c_high, c_low, b_high, b_low,
    turned_high, turned_low, cross_high, cross_low, solved_high, solved_low,
    part, landing, line, line_in, full, swapped,
    in_sems, send_sems, recv_sems,
):
    z, x, y = (lax.axis_index(name) for name in ROWS)
    core = lax.axis_index("tgt")
    place = x * NY + y
    rows = samples.shape[0]
    tiles = rows // TILE
    blocks, block = ids.shape
    mine = block // 2
    unit = part.shape[1]
    piece = unit // PLANE
    wide = targets.shape[1]

    def plane_peer(step):
        px, py = lax.rem(x + step[0], NX), lax.rem(y + step[1], NY)
        return (z, px, py, core), px * NY + py

    def line_peer(step):
        return (lax.rem(z + step, NZ), x, y, core)

    partner = (z, x, y, 1 - core)

    barrier = pltpu.get_barrier_semaphore()
    for step in LINE_STEPS:
        pl.semaphore_signal(barrier, inc=1, device_id=line_peer(step), device_id_type=MESH)
    for step in PLANE_STEPS:
        pl.semaphore_signal(barrier, inc=1, device_id=plane_peer(step)[0], device_id_type=MESH)
    pl.semaphore_signal(barrier, inc=1, device_id=partner, device_id_type=MESH)

    chunk = rows // CHUNKS
    counts_copy = pltpu.make_async_copy(counts_in, counts, in_sems.at[CHUNKS + 3])
    ids_copy = pltpu.make_async_copy(ids_in, ids, in_sems.at[CHUNKS])
    targets_copy = pltpu.make_async_copy(targets_in, targets, in_sems.at[CHUNKS + 1])
    inverse_copy = pltpu.make_async_copy(inverse_in, inverse, in_sems.at[CHUNKS + 2])

    def samples_copy(n):
        at = pl.ds(n * chunk, chunk)
        return pltpu.make_async_copy(samples_in.at[at], samples.at[at], in_sems.at[n])

    counts_copy.start()
    ids_copy.start()
    for n in range(CHUNKS):
        samples_copy(n).start()
    targets_copy.start()
    inverse_copy.start()

    def remote(src, dst, stage, device):
        return pltpu.make_async_remote_copy(
            src_ref=src, dst_ref=dst, send_sem=send_sems.at[stage], recv_sem=recv_sems.at[stage],
            device_id=device, device_id_type=MESH,
        )

    def arrived(u, n, ref):
        pltpu.make_async_copy(ref, ref, recv_sems.at[4 * u + n]).wait()

    def sent(u, n, ref):
        pltpu.make_async_copy(ref, ref, send_sems.at[4 * u + n]).wait()

    own_piece = pl.ds(pl.multiple_of(place * piece, piece), piece)

    def scatter(u):
        for slot, step in enumerate(PLANE_STEPS):
            device, index = plane_peer(step)
            src = part.at[u, pl.ds(pl.multiple_of(index * piece, piece), piece)]
            remote(src, landing.at[u, slot], 4 * u, device).start()

    def to_line(u):
        arrived(u, 0, landing.at[u])
        total = part[u, own_piece]
        for slot in range(PLANE - 1):
            total = total + landing[u, slot]
        line[u] = total
        for slot, step in enumerate(LINE_STEPS):
            remote(line.at[u], line_in.at[u, slot], 4 * u + 1, line_peer(step)).start()

    def off_line(u):
        arrived(u, 1, line_in.at[u])
        total = line[u]
        for slot in range(NZ - 1):
            total = total + line_in[u, slot]
        return total

    def gather(u, value):
        full[u, own_piece] = value
        ref = full.at[u, own_piece]
        for step in PLANE_STEPS:
            remote(ref, ref, 4 * u + 2, plane_peer(step)[0]).start()

    def gathered(u):
        arrived(u, 2, landing.at[u])

    def swap(u):
        gathered(u)
        remote(full.at[u], swapped.at[u], 4 * u + 3, partner).start()

    per_chunk = tiles // CHUNKS
    for n in range(CHUNKS):
        samples_copy(n).wait()

        def split_samples(i, carry):
            at = tile_at(i)
            x_high[at], x_low[at] = halves(samples[at])
            return carry

        lax.fori_loop(n * per_chunk, (n + 1) * per_chunk, split_samples, 0)
    ids_copy.wait()
    counts_copy.wait()

    first = ((z * NX + x) * NY + y) * rows

    def pick(b):
        wanted = ids[pl.ds(b, 1), pl.ds(pl.multiple_of(core * mine, mine), mine)] - first
        column = jnp.broadcast_to(wanted.astype(f32), (8, mine)).T[:, :1]
        slots = lax.broadcasted_iota(jnp.int32, (mine, rows), 1).astype(f32)
        chosen = jnp.where(column == slots, 1.0, 0.0).astype(bf16)
        value = dot(chosen, x_high[...], NN) + dot(chosen, x_low[...], NN)
        for n in range(2):
            part[2 * b + n] = value[n * unit:(n + 1) * unit]

    pick(0)
    pl.semaphore_wait(barrier, PLANE + NZ - 1)
    scatter(0)
    scatter(1)
    pick(1)

    targets_copy.wait()

    def turn_targets(i, carry):
        at = tile_at(i)
        high, low = halves(targets[at].T)
        r_turned[pl.ds(0, wide), at] = high
        r_turned[pl.ds(wide, wide), at] = low
        return carry

    lax.fori_loop(0, tiles, turn_targets, 0)

    inverse_copy.wait()
    for b in range(blocks):
        for i in range(2):
            for j in range(2):
                from_i = pl.ds(pl.multiple_of((core + i) % 2 * mine, mine), mine)
                from_j = pl.ds(pl.multiple_of((core + j) % 2 * mine, mine), mine)
                high, low = halves(inverse[b, from_i, from_j])
                b_high[b, pl.ds(i * mine, mine), pl.ds(j * mine, mine)] = high
                b_low[b, pl.ds(i * mine, mine), pl.ds(j * mine, mine)] = low

    to_line(0)
    to_line(1)
    scatter(2)
    scatter(3)
    gather(0, off_line(0))
    gather(1, off_line(1))
    to_line(2)
    to_line(3)

    scale = 0.5 / samples.shape[1] ** 0.5

    def points_ready(b, h):
        for n in range(2):
            u = 2 * b + n
            if h == 1:
                arrived(u, 3, swapped.at[u])
            value = swapped[u] if h == 1 else full[u]
            at = pl.ds(h * mine + n * unit, unit)
            p_high[b, at], p_low[b, at] = halves(value * scale)

    live = counts[0]

    def columns(b, h, i):
        at, points = tile_at(i), pl.ds(h * mine, mine)
        high, low = p_high[b, points], p_low[b, points]
        near = (dot(x_high[at], high, NT) + dot(x_high[at], low, NT) + dot(x_low[at], high, NT)) + 1.0
        slots = i * TILE + lax.broadcasted_iota(jnp.int32, near.shape, 0)
        cubed = jnp.where(slots < live, near * near * near, 0.0)
        c_high[b, at, points], c_low[b, at, points] = halves(cubed)
        return cubed

    def sums(b, h):
        points = pl.ds(h * mine, mine)
        both = dot(r_turned[...], c_high[b, :, points], NN)
        value = both[:wide] + both[wide:] + dot(r_turned[pl.ds(0, wide)], c_low[b, :, points], NN)
        part[2 * (blocks + b) + h] = value

    def update(u, i, current):
        b, h = u // 2 - blocks, u % 2
        points = pl.ds(h * mine, mine)
        high, low = halves(full[u])
        both = dot(c_high[b, tile_at(i), points], jnp.concatenate([high, low], axis=0), NT)
        return current - (both[:, :wide] + both[:, wide:] + dot(c_low[b, tile_at(i), points], high, NT))

    def coefs():
        sums = jnp.concatenate([off_line(4), off_line(5)], axis=1)
        high, low = halves(sums)
        both = jnp.concatenate([high, low], axis=0)
        for h in range(2):
            at = pl.ds(h * mine, mine)
            value = dot(both, b_high[0, at], NT)
            gather(4 + h, value[:piece] + value[piece:] + dot(high, b_low[0, at], NT))

    swap(0)
    swap(1)
    points_ready(0, 0)
    gather(2, off_line(2))
    gather(3, off_line(3))

    for h in range(2):
        if h == 1:
            points_ready(0, 1)
        for i in range(tiles):
            columns(0, h, i)
        sums(0, h)
        scatter(4 + h)

    def second_columns(h):
        points_ready(1, h)
        for i in range(tiles):
            high, low = halves(columns(1, h, i).T)
            turned_high[pl.ds(h * mine, mine), tile_at(i)] = high
            turned_low[pl.ds(h * mine, mine), tile_at(i)] = low

    def cross(h):
        at = pl.ds(h * mine, mine)
        value = (
            dot(turned_high[at], c_high[0], NN)
            + dot(turned_high[at], c_low[0], NN)
            + dot(turned_low[at], c_high[0], NN)
        )
        cross_high[at], cross_low[at] = halves(value)

    swap(2)
    swap(3)
    second_columns(0)
    second_columns(1)
    to_line(4)
    to_line(5)
    cross(0)
    cross(1)
    coefs()
    sums(1, 0)
    sums(1, 1)

    early_high, early_low = halves(jnp.concatenate([part[6], part[7]], axis=1))
    for h in range(2):
        at = pl.ds(h * mine, mine)
        solved_high[at], solved_low[at] = halves(
            dot(b_high[1, at], cross_high[...], NN)
            + dot(b_high[1, at], cross_low[...], NN)
            + dot(b_low[1, at], cross_high[...], NN)
        )
        part[6 + h] = (
            dot(early_high, b_high[1, at], NT) + dot(early_high, b_low[1, at], NT) + dot(early_low, b_high[1, at], NT)
        )

    gathered(4)
    gathered(5)
    high, low = halves(jnp.concatenate([full[4], full[5]], axis=1))
    both = jnp.concatenate([high, low], axis=0)
    for h in range(2):
        at = pl.ds(h * mine, mine)
        value = dot(both, solved_high[at], NT)
        part[6 + h] -= value[:wide] + value[wide:] + dot(high, solved_low[at], NT)
        scatter(6 + h)

    for i in range(tiles):
        at = tile_at(i)
        residual[at] = update(5, i, update(4, i, targets[at]))
    to_line(6)
    to_line(7)
    gather(6, off_line(6))
    gather(7, off_line(7))
    gathered(6)
    for i in range(tiles):
        at = tile_at(i)
        residual[at] = update(6, i, residual[at])
    gathered(7)
    for i in range(tiles):
        at = tile_at(i)
        out[at] = update(7, i, residual[at])

    for u in range(4 * blocks):
        sent(u, 0, landing.at[u])
        sent(u, 1, line_in.at[u])
        sent(u, 2, landing.at[u])
        if u < 2 * blocks:
            sent(u, 3, swapped.at[u])


def on_device(counts, samples, targets, point_ids, block_inverse):
    rows, feat = samples.shape
    blocks, block = point_ids.shape
    wide = targets.shape[1]
    units, unit, lanes = 4 * blocks, block // 4, block // 2
    piece = unit // PLANE
    anywhere = pl.BlockSpec(memory_space=pl.ANY)
    return pl.pallas_call(
        kernel,
        out_shape=pltpu.VMEM(targets.shape, f32),
        in_specs=[anywhere] * 5,
        out_specs=pl.BlockSpec(memory_space=pltpu.VMEM),
        scratch_shapes=[
            pltpu.SMEM(counts.shape, jnp.int32),
            pltpu.VMEM(point_ids.shape, jnp.int32),
            pltpu.VMEM((rows, feat), f32),
            pltpu.VMEM((rows, wide), f32),
            pltpu.VMEM((blocks, block, block), f32),
            pltpu.VMEM((rows, feat), bf16),
            pltpu.VMEM((rows, feat), bf16),
            pltpu.VMEM((2 * wide, rows), bf16),
            pltpu.VMEM((rows, wide), f32),
            pltpu.VMEM((blocks, block, feat), bf16),
            pltpu.VMEM((blocks, block, feat), bf16),
            pltpu.VMEM((blocks, rows, block), bf16),
            pltpu.VMEM((blocks, rows, block), bf16),
            pltpu.VMEM((blocks, block, block), bf16),
            pltpu.VMEM((blocks, block, block), bf16),
            pltpu.VMEM((block, rows), bf16),
            pltpu.VMEM((block, rows), bf16),
            pltpu.VMEM((block, block), bf16),
            pltpu.VMEM((block, block), bf16),
            pltpu.VMEM((block, block), bf16),
            pltpu.VMEM((block, block), bf16),
            pltpu.VMEM((units, unit, lanes), f32),
            pltpu.VMEM((units, PLANE - 1, piece, lanes), f32),
            pltpu.VMEM((units, piece, lanes), f32),
            pltpu.VMEM((units, NZ - 1, piece, lanes), f32),
            pltpu.VMEM((units, unit, lanes), f32),
            pltpu.VMEM((2 * blocks, unit, lanes), f32),
            pltpu.SemaphoreType.DMA((CHUNKS + 4,)),
            pltpu.SemaphoreType.DMA((4 * units,)),
            pltpu.SemaphoreType.DMA((4 * units,)),
        ],
        compiler_params=pltpu.CompilerParams(collective_id=0, has_side_effects=True),
    )(counts, point_ids, samples, targets, block_inverse)


def solution(mesh):
    finer = Mesh(
        mesh.devices.reshape(NZ, NX, NY, mesh.shape["tgt"]), ("rows_0", "rows_1", "rows_2", "tgt")
    )
    placed = (P(ROWS), P(ROWS, None), P(ROWS, "tgt"), P(), P())
    return jax.shard_map(
        on_device, mesh=finer, in_specs=placed, out_specs=P(ROWS, "tgt"), check_vma=False
    )
```
